32 devices in a mesh: dp: 4 (over x, y), ep: 8 (over z, core).
Axes of the slice: x: 2, y: 2, z: 4, core: 2. Of those that a mesh axis runs over, the one named last changes fastest.
Arguments:
- x: bfloat16 [4, 8, 256, 2048], P('dp', 'ep'), parts along dimension 0
- expert: int32 [4, 8, 256, 2], P('dp', 'ep'), parts along dimension 0
- slot: int32 [4, 8, 256, 2], P('dp', 'ep'), parts along dimension 0
- gate: float32 [4, 8, 256, 2], P('dp', 'ep'), parts along dimension 0
- w_gate: bfloat16 [8, 2048, 5632], P('ep')
- w_up: bfloat16 [8, 2048, 5632], P('ep')
- w_down: bfloat16 [8, 5632, 2048], P('ep')
Outputs:
- y: bfloat16 [4, 8, 256, 2048], P('dp', 'ep'), parts along dimension 0
There are 4 independent parts. The reference program is written for one: setup_inputs(seed, part) draws one part's arguments, and reference() takes and returns one part's arrays. A program takes and returns all parts, laid end to end along the dimension named above; an argument that names none is the same for every part.
All inputs are finite; a program needn't handle non-finite values.
Results may differ from the reference program's by a relative error of at most 0.009.
Values are sent between devices in bfloat16 or wider.
A program may use at most 2 GiB of HBM per device.

```python
import jax
import jax.numpy as jnp

MEMBERS = 8
TOKENS = 256
D = 2048
FF = 5632
TOP = 2
EXPERTS = 8
SLOTS = 5 * TOKENS * TOP // (4 * EXPERTS)


def setup_inputs(seed: int = 0, part: int = 0) -> dict:
    own, k1, k2, k3, k4, k5, k6 = jax.random.split(jax.random.key(seed), 7)
    kx, ke, kl, kg = jax.random.split(jax.random.fold_in(own, part), 4)
    devices = (1, MEMBERS)
    place = jax.random.permutation(kl, jnp.arange(EXPERTS, dtype=jnp.uint32))
    slow = ((EXPERTS + (9 * place) % EXPERTS) << ((9 * place) // EXPERTS)) // EXPERTS
    wait = (jax.random.bits(ke, (*devices, TOKENS, EXPERTS), jnp.uint32) >> 10) * slow
    expert = jnp.argsort(wait, axis=-1)[..., :TOP].astype(jnp.int32)
    chosen = jax.nn.one_hot(expert, EXPERTS, dtype=jnp.int32)
    in_line = jnp.cumsum(chosen.reshape(*devices, TOKENS * TOP, EXPERTS), axis=2) - 1
    slot = jnp.sum(in_line.reshape(chosen.shape) * chosen, axis=-1)

    def one(key, rows, columns):
        return (jax.random.normal(key, (rows, columns), jnp.float32) * rows**-0.5).astype(jnp.bfloat16)

    def weights(key, rows, columns):
        return jax.lax.map(lambda k: one(k, rows, columns), jax.random.split(key, EXPERTS))

    return {
        "x": jax.random.normal(kx, (*devices, TOKENS, D), jnp.float32).astype(jnp.bfloat16),
        "expert": expert,
        "slot": slot,
        "gate": jax.nn.softmax(jax.random.normal(kg, expert.shape, jnp.float32)),
        "w_gate": weights(k1, D, FF),
        "w_up": weights(k2, D, FF),
        "w_down": weights(k3, FF, D),
    }


def einsum(form, a, b):
    return jnp.einsum(form, a.astype(jnp.float32), b.astype(jnp.float32))


def reference(x, expert, slot, gate, w_gate, w_up, w_down):
    to_expert = jax.nn.one_hot(expert, EXPERTS, dtype=jnp.bfloat16)
    to_slot = jax.nn.one_hot(slot, SLOTS, dtype=jnp.bfloat16)
    weighted = to_expert * gate[..., None].astype(jnp.bfloat16)
    dispatch = einsum("abtke,abtkc->abtec", to_expert, to_slot).astype(jnp.bfloat16)
    combine = einsum("abtke,abtkc->abtec", weighted, to_slot).astype(jnp.bfloat16)
    z = einsum("abtec,abtd->aebcd", dispatch, x).astype(jnp.bfloat16)
    h = jax.nn.silu(einsum("aebcd,edf->aebcf", z, w_gate))
    h = (h * einsum("aebcd,edf->aebcf", z, w_up)).astype(jnp.bfloat16)
    out = einsum("aebcf,efd->aebcd", h, w_down).astype(jnp.bfloat16)
    y = einsum("abtec,aebcd->abtd", combine, out)
    return y.astype(jnp.bfloat16)
```

```python
import functools

import jax
import jax.numpy as jnp
from jax import lax
from jax.experimental import pallas as pl
from jax.experimental.pallas import tpu as pltpu
from jax.sharding import PartitionSpec as P

MESH = pl.DeviceIdType.MESH
F32, BF16 = jnp.float32, jnp.bfloat16
PIECES = 4
GU_TILES = 11
DN_TILES = 8
NBUF = 4


def kernel(slots, meta, x_hbm, wg, wu, wd, y_hbm,
           xv, xf, mf, oh, za, zb, stage, stagef, hbuf, oa, ob_, ro, rof,
           part, prt, yv, gbuf, ubuf, dbuf,
           xsem, gsem, usem, dsem, ysem, go,
           s_meta, s_x, s_own, s_rel, s_outa, s_outb, s_part,
           r_meta, r_x, r_za, r_zp, r_zb, r_zn, r_rof, r_ro, r_part):
    S = slots
    T, D = xv.shape
    FT = gbuf.shape[-1]
    NT = dbuf.shape[-1]
    C = D // PIECES
    HALF = 4 * S

    dp = lax.axis_index("dp")
    me = lax.axis_index("ep")
    z = lax.div(me, 2)
    k = lax.rem(me, 2)
    h = lax.div(me, 4)
    q = lax.rem(me, 4)
    mid = lax.rem(z + h, 2) == 1
    end = lax.rem(z + h, 2) == 0
    partner = 2 * z + 1 - k
    qp = partner - 4 * h
    other = 2 + 8 * h - 2 * z
    qo = other - 4 * h
    relay = 4 - 2 * h + k
    far_end = 6 - 6 * h + k
    base = h * HALF

    def rows(i):
        return pl.ds(pl.multiple_of(i * S, 16), S)

    def cols(p):
        return pl.ds(pl.multiple_of(p * C, 128), C)

    def send(src, dst, ssem, rsem, dev):
        return pltpu.make_async_remote_copy(
            src_ref=src, dst_ref=dst, send_sem=ssem, recv_sem=rsem,
            device_id=(dp, dev), device_id_type=MESH)

    def recv(dst, rsem):
        pltpu.make_async_remote_copy(
            src_ref=dst, dst_ref=dst, send_sem=rsem, recv_sem=rsem,
            device_id=(dp, partner), device_id_type=MESH).wait_recv()

    def gu_copies(t):
        slot = lax.rem(t, NBUF)
        tile = pl.ds(pl.multiple_of(lax.rem(t, GU_TILES) * FT, 128), FT)
        return (pltpu.make_async_copy(wg.at[:, tile], gbuf.at[slot], gsem.at[slot]),
                pltpu.make_async_copy(wu.at[:, tile], ubuf.at[slot], usem.at[slot]))

    def dn_copy(t):
        slot = lax.rem(t, NBUF)
        tile = pl.ds(pl.multiple_of(lax.rem(t, DN_TILES) * NT, 128), NT)
        return pltpu.make_async_copy(wd.at[:, tile], dbuf.at[slot], dsem.at[slot])

    xload = [pltpu.make_async_copy(x_hbm.at[:, cols(p)], xv.at[:, cols(p)], xsem.at[p])
             for p in range(PIECES)]
    for c in xload:
        c.start()
    for t in range(NBUF):
        for c in gu_copies(jnp.int32(t)):
            c.start()
    for t in range(NBUF):
        dn_copy(jnp.int32(t)).start()

    barrier = pltpu.get_barrier_semaphore()
    for d in range(1, 8):
        pl.semaphore_signal(barrier, inc=1, device_id=(dp, lax.rem(me + d, 8)), device_id_type=MESH)

    def onehot(m):
        idx = m[...].astype(jnp.int32) - base
        r = lax.broadcasted_iota(jnp.int32, (HALF, T), 0)
        hit = (r == idx[0:1, :]) | (r == idx[1:2, :])
        return jnp.where(hit, 1.0, 0.0).astype(BF16)

    def weights_of(m):
        mt = jnp.transpose(jnp.concatenate([m[...], jnp.zeros((120, T), F32)], axis=0))
        idx = mt.astype(jnp.int32) - base
        r = lax.broadcasted_iota(jnp.int32, (T, HALF), 1)
        w = jnp.where(r == idx[:, 0:1], mt[:, 2:3], 0.0)
        w = jnp.where(r == idx[:, 1:2], mt[:, 3:4], w)
        return w.astype(BF16)

    def dot(a, b):
        return jnp.dot(a, b, preferred_element_type=F32)

    oh[0] = onehot(meta)
    pl.semaphore_wait(barrier, 7)

    side = lax.rem(z + h + 1, 2)

    def send_x(p):
        return send(xv.at[:, cols(p)], xf.at[side, :, cols(p)], s_x.at[p], r_x.at[side, p], relay)

    def own_copies(p):
        a = send(stage.at[rows(qp), cols(p)], za.at[rows(2 + k), cols(p)], s_own.at[0, p], r_zp.at[p], partner)
        b = [send(stage.at[rows(qo + j), cols(p)], zb.at[rows(2 + k), cols(p)], s_own.at[1 + j, p],
                  r_zn.at[k, p], other + j) for j in range(2)]
        return a, b

    send_meta = send(meta, mf.at[side], s_meta, r_meta.at[side], relay)
    send_meta.start()
    for p in range(PIECES):
        xload[p].wait()

        @pl.when(mid)
        def _(p=p):
            send_x(p).start()

    for p in range(PIECES):
        stage[:, cols(p)] = dot(oh[0], xv[:, cols(p)]).astype(BF16)
        za[rows(2 + k), cols(p)] = stage[rows(q), cols(p)]
        a, b = own_copies(p)
        a.start()
        if p < 2:
            for c in b:
                c.start()
        else:
            @pl.when(end)
            def _(b=b):
                for c in b:
                    c.start()

    def relay_copies(f, p):
        zx = za if f == 0 else zb
        rz = r_za if f == 0 else r_zb
        return [send(stagef.at[f, rows(qd), cols(p)], zx.at[rows(k), cols(p)], s_rel.at[f, j, p],
                     rz.at[k, p], dev)
                for j, (qd, dev) in enumerate(((qo, other), (qo + 1, other + 1), (qp, partner)))]

    def relay_piece(f, p):
        zx = za if f == 0 else zb
        recv(xf.at[f, :, cols(p)], r_x.at[f, p])
        stagef[f, :, cols(p)] = dot(oh[1 + f], xf[f, :, cols(p)]).astype(BF16)
        for c in relay_copies(f, p):
            c.start()
        zx[rows(k), cols(p)] = stagef[f, rows(q), cols(p)]

    def relay_head(f):
        recv(mf.at[f], r_meta.at[f])
        oh[1 + f] = onehot(mf.at[f])

    @pl.when(mid)
    def _():
        relay_head(0)
        for p in range(PIECES):
            relay_piece(0, p)
            if p == PIECES - 2:
                pl.semaphore_signal(go, inc=1, device_id=(dp, far_end), device_id_type=MESH)
        for p in range(2, PIECES):
            for c in own_copies(p)[1]:
                c.start()

    @pl.when(end)
    def _():
        pl.semaphore_wait(go, 1)
        for p in range(PIECES):
            send_x(p).start()
        for p in range(PIECES):
            recv(za.at[rows(k), cols(p)], r_za.at[k, p])

    for p in range(PIECES):
        recv(za.at[rows(1 - k), cols(p)], r_za.at[1 - k, p])
        recv(za.at[rows(3 - k), cols(p)], r_zp.at[p])

    def gu_tile(zx, t, i):
        for c in gu_copies(t):
            c.wait()
        slot = lax.rem(t, NBUF)

        @pl.when((t >= 1) & (t + NBUF - 1 < 2 * GU_TILES))
        def _():
            for c in gu_copies(t + NBUF - 1):
                c.start()

        g = dot(zx[...], gbuf[slot])
        u = dot(zx[...], ubuf[slot])
        hbuf[:, pl.ds(pl.multiple_of(i * FT, 128), FT)] = (g * jax.nn.sigmoid(g) * u).astype(BF16)

    def dn_tile(ox, t, n):
        dn_copy(t).wait()
        slot = lax.rem(t, NBUF)

        @pl.when((t >= 1) & (t + NBUF - 1 < 2 * DN_TILES))
        def _():
            dn_copy(t + NBUF - 1).start()

        ox[:, pl.ds(pl.multiple_of(n * NT, 128), NT)] = dot(hbuf[...], dbuf[slot]).astype(BF16)

    def out_far(f, p, start):
        ox = oa if f == 0 else ob_
        ss = s_outa if f == 0 else s_outb

        def to(kk, dev):
            return send(ox.at[rows(kk), cols(p)], rof.at[f, rows(q), cols(p)], ss.at[kk, p],
                        r_rof.at[f, q, p], dev)

        @pl.when(mid)
        def _():
            c = to(1 - k, partner)
            if start:
                c.start()
                rof[f, rows(q), cols(p)] = ox[rows(k), cols(p)]
            else:
                c.wait_send()

        @pl.when(end)
        def _():
            for kk in range(2):
                c = to(kk, other + kk)
                c.start() if start else c.wait_send()

    def out_near_a(p):
        return send(oa.at[rows(3 - k), cols(p)], ro.at[rows(q), cols(p)], s_outa.at[2, p], r_ro.at[q, p], partner)

    def out_near_b(p):
        return [send(ob_.at[rows(2 + j), cols(p)], ro.at[rows(q), cols(p)], s_outb.at[2 + j, p],
                     r_ro.at[q, p], other + j) for j in range(2)]

    def send_part(f, p):
        dev = relay if f == 0 else far_end
        return send(prt.at[f, :, cols(p)], part.at[:, cols(p)], s_part.at[f, p], r_part.at[p], dev)

    def combine_piece(f, p):
        for qq in (qp, qo, qo + 1):
            recv(rof.at[f, rows(qq), cols(p)], r_rof.at[f, qq, p])
        prt[f, :, cols(p)] = dot(weights_of(mf.at[f]), rof[f, :, cols(p)]).astype(BF16)
        send_part(f, p).start()

    @pl.loop(0, GU_TILES)
    def _(i):
        gu_tile(za, i, i)

        @pl.when(mid & (i == 2))
        def _():
            relay_head(1)

        @pl.when(mid & (lax.rem(i, 4) == 3))
        def _():
            relay_piece(1, lax.div(i, 4))

    @pl.loop(0, DN_TILES)
    def _(n):
        @pl.when(mid & (lax.rem(n, 5) == 0))
        def _():
            relay_piece(1, 2 + lax.div(n, 5))

        dn_tile(oa, n, n)

        @pl.when(lax.rem(n, 2) == 1)
        def _():
            p = lax.div(n, 2)
            out_far(0, p, True)
            out_near_a(p).start()
            ro[rows(q), cols(p)] = oa[rows(2 + k), cols(p)]

    @pl.when(end)
    def _():
        for p in range(PIECES):
            recv(zb.at[rows(k), cols(p)], r_zb.at[k, p])

    for p in range(PIECES):
        recv(zb.at[rows(1 - k), cols(p)], r_zb.at[1 - k, p])
        for j in range(2):
            recv(zb.at[rows(2 + j), cols(p)], r_zn.at[j, p])

    @pl.loop(0, GU_TILES)
    def _(i):
        @pl.when(mid & (lax.rem(i, 3) == 0))
        def _():
            combine_piece(0, lax.div(i, 3))

        gu_tile(zb, GU_TILES + i, i)

    @pl.loop(0, DN_TILES)
    def _(n):
        dn_tile(ob_, DN_TILES + n, n)

        @pl.when(lax.rem(n, 2) == 1)
        def _():
            out_far(1, lax.div(n, 2), True)

    for p in range(PIECES):
        for c in out_near_b(p):
            c.start()

    @pl.when(mid)
    def _():
        for p in range(PIECES):
            combine_piece(1, p)

    ycopy = [pltpu.make_async_copy(yv.at[:, cols(p)], y_hbm.at[:, cols(p)], ysem.at[p]) for p in range(PIECES)]
    w_own = weights_of(meta)
    for p in range(PIECES):
        recv(ro.at[rows(qp), cols(p)], r_ro.at[qp, p])
        for j in range(2):
            recv(ro.at[rows(qo + j), cols(p)], r_ro.at[qo + j, p])
        recv(part.at[:, cols(p)], r_part.at[p])
        yv[:, cols(p)] = (dot(w_own, ro[:, cols(p)]) + part[:, cols(p)].astype(F32)).astype(BF16)
        ycopy[p].start()

    send_meta.wait_send()
    for p in range(PIECES):
        send_x(p).wait_send()
        a, b = own_copies(p)
        for c in (a, *b, out_near_a(p), *out_near_b(p)):
            c.wait_send()
        for f in range(2):
            out_far(f, p, False)

    @pl.when(mid)
    def _():
        for p in range(PIECES):
            for f in range(2):
                for c in relay_copies(f, p):
                    c.wait_send()
                send_part(f, p).wait_send()

    for c in ycopy:
        c.wait()


def solution(mesh):
    def step(x, expert, slot, gate, w_gate, w_up, w_down):
        tokens, depth = x.shape[2:]
        ff = w_gate.shape[2]
        top = expert.shape[3]
        slots = 5 * tokens * top // (4 * 8)
        place = jnp.where(slot < slots, expert * slots + slot, -100000).astype(F32)
        meta = jnp.concatenate([place.reshape(tokens, top), gate.reshape(tokens, top),
                                jnp.zeros((tokens, 8 - 2 * top), F32)], axis=1).T
        half = 4 * slots
        dma = pltpu.SemaphoreType.DMA
        vmem = pltpu.VMEM
        hbm = pl.BlockSpec(memory_space=pl.ANY)
        y = pl.pallas_call(
            functools.partial(kernel, slots),
            out_shape=jax.ShapeDtypeStruct((tokens, depth), BF16),
            in_specs=[pl.BlockSpec(memory_space=pltpu.VMEM)] + [hbm] * 4,
            out_specs=hbm,
            scratch_shapes=[
                vmem((tokens, depth), BF16),
                vmem((2, tokens, depth), BF16),
                vmem((2, 8, tokens), F32),
                vmem((3, half, tokens), BF16),
                vmem((half, depth), BF16),
                vmem((half, depth), BF16),
                vmem((half, depth), BF16),
                vmem((2, half, depth), BF16),
                vmem((half, ff), BF16),
                vmem((half, depth), BF16),
                vmem((half, depth), BF16),
                vmem((half, depth), BF16),
                vmem((2, half, depth), BF16),
                vmem((tokens, depth), BF16),
                vmem((2, tokens, depth), BF16),
                vmem((tokens, depth), BF16),
                vmem((NBUF, depth, ff // GU_TILES), BF16),
                vmem((NBUF, depth, ff // GU_TILES), BF16),
                vmem((NBUF, ff, depth // DN_TILES), BF16),
                dma((PIECES,)), dma((NBUF,)), dma((NBUF,)), dma((NBUF,)), dma((PIECES,)),
                pltpu.SemaphoreType.REGULAR,
                dma, dma((PIECES,)), dma((3, PIECES)), dma((2, 3, PIECES)),
                dma((3, PIECES)), dma((4, PIECES)), dma((2, PIECES)),
                dma((2,)), dma((2, PIECES)), dma((2, PIECES)), dma((PIECES,)),
                dma((2, PIECES)), dma((2, PIECES)), dma((2, 4, PIECES)), dma((4, PIECES)), dma((PIECES,)),
            ],
            compiler_params=pltpu.CompilerParams(
                collective_id=0, has_side_effects=True, vmem_limit_bytes=67043328),
        )(meta, x.reshape(tokens, depth), w_gate[0], w_up[0], w_down[0])
        return y.reshape(x.shape)

    tok = P("dp", "ep")
    return jax.shard_map(step, mesh=mesh, in_specs=(tok,) * 4 + (P("ep"),) * 3, out_specs=tok, check_vma=False)
```

```python
import functools

import jax
import jax.numpy as jnp
from jax import lax
from jax.experimental import pallas as pl
from jax.experimental.pallas import tpu as pltpu
from jax.sharding import PartitionSpec as P

MESH = pl.DeviceIdType.MESH
F32, BF16 = jnp.float32, jnp.bfloat16
PIECES = 4
NBUF = 4
DBUF = 2


def kernel(slots, expert, slot, gate, x_hbm, wg, wu, wd, y_hbm,
           meta, xv, xf, mf, oh, wt, za, zb, stage, stagef, acc, hbuf, ro, rof,
           part, kbuf, dbuf,
           xsem, ksem, dsem, ysem, go,
           s_meta, s_x, s_own, s_rel, s_outa, s_outb, s_part,
           r_meta, r_x, r_za, r_zp, r_zn, r_zb, r_rof, r_ro, r_part):
    S = slots
    T, D = xv.shape
    FF = hbuf.shape[1]
    KT, FT = kbuf.shape[1:]
    NT = dbuf.shape[2]
    C = D // PIECES
    HALF = 4 * S
    NF = FF // FT
    GU = 2 * NF * PIECES

    dp = lax.axis_index("dp")
    me = lax.axis_index("ep")
    z = lax.div(me, 2)
    k = lax.rem(me, 2)
    h = lax.div(me, 4)
    q = lax.rem(me, 4)
    side = lax.rem(z + h + 1, 2)
    mid = side == 0
    end = side == 1
    partner = 2 * z + 1 - k
    qp = partner - 4 * h
    other = 2 + 8 * h - 2 * z
    qo = other - 4 * h
    relay = 4 - 2 * h + k
    far_end = 6 - 6 * h + k
    base = h * HALF

    def rows(i):
        return pl.ds(pl.multiple_of(i * S, 16), S)

    def cols(p):
        return pl.ds(pl.multiple_of(p * C, 128), C)

    def send(src, dst, ssem, rsem, dev):
        return pltpu.make_async_remote_copy(
            src_ref=src, dst_ref=dst, send_sem=ssem, recv_sem=rsem,
            device_id=(dp, dev), device_id_type=MESH)

    def recv(dst, rsem):
        pltpu.make_async_remote_copy(
            src_ref=dst, dst_ref=dst, send_sem=rsem, recv_sem=rsem,
            device_id=(dp, partner), device_id_type=MESH).wait_recv()

    def gu_copy(t, w, m):
        t = lax.rem(t, GU)
        r = pl.ds(pl.multiple_of(lax.div(t, 2 * NF) * KT, 128), KT)
        c = pl.ds(pl.multiple_of(lax.div(lax.rem(t, 2 * NF), 2) * FT, 128), FT)
        return w.at[r, c]

    def gu_start(t):
        s = lax.rem(t, NBUF)

        @pl.when(lax.rem(t, 2) == 0)
        def _():
            pltpu.make_async_copy(gu_copy(t, wg, 0), kbuf.at[s], ksem.at[s]).start()

        @pl.when(lax.rem(t, 2) == 1)
        def _():
            pltpu.make_async_copy(gu_copy(t, wu, 1), kbuf.at[s], ksem.at[s]).start()

    def gu_wait(t):
        s = lax.rem(t, NBUF)
        pltpu.make_async_copy(gu_copy(t, wg, 0), kbuf.at[s], ksem.at[s]).wait()
        return s

    def dn_copy(t):
        s = lax.rem(t, DBUF)
        tile = pl.ds(pl.multiple_of(lax.rem(t, PIECES) * NT, 128), NT)
        return pltpu.make_async_copy(wd.at[:, tile], dbuf.at[s], dsem.at[s])

    xload = [pltpu.make_async_copy(x_hbm.at[:, cols(p)], xv.at[:, cols(p)], xsem.at[p])
             for p in range(PIECES)]
    for c in xload:
        c.start()
    for t in range(NBUF):
        gu_start(jnp.int32(t))
    for t in range(DBUF):
        dn_copy(jnp.int32(t)).start()

    barrier = pltpu.get_barrier_semaphore()
    for d in range(1, 8):
        pl.semaphore_signal(barrier, inc=1, device_id=(dp, lax.rem(me + d, 8)), device_id_type=MESH)

    def onehot(m):
        idx = m[...].astype(jnp.int32) - base
        r = lax.broadcasted_iota(jnp.int32, (HALF, T), 0)
        hit = (r == idx[0:1, :]) | (r == idx[1:2, :])
        return jnp.where(hit, 1.0, 0.0).astype(BF16)

    def weights_of(m):
        mt = jnp.transpose(jnp.concatenate([m[...], jnp.zeros((120, T), F32)], axis=0))
        idx = mt.astype(jnp.int32) - base
        r = lax.broadcasted_iota(jnp.int32, (T, HALF), 1)
        w = jnp.where(r == idx[:, 0:1], mt[:, 2:3], 0.0)
        w = jnp.where(r == idx[:, 1:2], mt[:, 3:4], w)
        return w.astype(BF16)

    def dot(a, b):
        return jnp.dot(a, b, preferred_element_type=F32)

    meta[...] = jnp.zeros_like(meta)
    meta[0:2, :] = jnp.where(slot[...] < S, expert[...] * S + slot[...], -100000).astype(F32)
    meta[2:4, :] = gate[...]
    oh[0] = onehot(meta)
    wt[0] = weights_of(meta)
    pl.semaphore_wait(barrier, 7)

    send_meta = send(meta, mf.at[side], s_meta, r_meta.at[side], relay)

    def send_x(p):
        return send(xv.at[:, cols(p)], xf.at[side, :, cols(p)], s_x.at[p], r_x.at[side, p], relay)

    def own_copies(p):
        a = send(stage.at[rows(qp), cols(p)], zb.at[rows(2 + k), cols(p)], s_own.at[0, p], r_zp.at[p], partner)
        b = [send(stage.at[rows(qo + j), cols(p)], za.at[rows(2 + k), cols(p)], s_own.at[1 + j, p],
                  r_zn.at[k, p], other + j) for j in range(2)]
        return a, b

    send_meta.start()
    for p in range(PIECES):
        xload[p].wait()

        @pl.when(mid)
        def _(p=p):
            send_x(p).start()

    for p in range(PIECES):
        stage[:, cols(p)] = dot(oh[0], xv[:, cols(p)]).astype(BF16)
        a, b = own_copies(p)
        if p < 2:
            for c in b:
                c.start()
        else:
            @pl.when(end)
            def _(b=b):
                for c in b:
                    c.start()
        a.start()
        zb[rows(2 + k), cols(p)] = stage[rows(q), cols(p)]

    def relay_copies(f, p):
        zx, rz = (za, r_za) if f == 0 else (zb, r_zb)
        return [send(stagef.at[f, rows(qd), cols(p)], zx.at[rows(k), cols(p)], s_rel.at[f, j, p],
                     rz.at[k, p], dev)
                for j, (qd, dev) in enumerate(((qo, other), (qo + 1, other + 1), (qp, partner)))]

    def relay_piece(f, p):
        zx = za if f == 0 else zb
        if p == 0:
            recv(mf.at[f], r_meta.at[f])
            oh[1 + f] = onehot(mf.at[f])
        recv(xf.at[f, :, cols(p)], r_x.at[f, p])
        stagef[f, :, cols(p)] = dot(oh[1 + f], xf[f, :, cols(p)]).astype(BF16)
        for c in relay_copies(f, p):
            c.start()
        zx[rows(k), cols(p)] = stagef[f, rows(q), cols(p)]
        if p == PIECES - 1:
            wt[1 + f] = weights_of(mf.at[f])

    def await_z(f, p):
        zx, rz = (za, r_za) if f == 0 else (zb, r_zb)

        @pl.when(end)
        def _():
            recv(zx.at[rows(k), cols(p)], rz.at[k, p])

        recv(zx.at[rows(1 - k), cols(p)], rz.at[1 - k, p])
        if f == 0:
            for j in range(2):
                recv(za.at[rows(2 + j), cols(p)], r_zn.at[j, p])
        else:
            recv(zb.at[rows(3 - k), cols(p)], r_zp.at[p])

    def ft(c):
        return pl.ds(pl.multiple_of(c * FT, 128), FT)

    def gu_next(t):
        @pl.when(t + NBUF < 2 * GU)
        def _():
            gu_start(t + NBUF)

    def gu_piece(f, p, hooks=()):
        zx = za if f == 0 else zb
        t0 = f * GU + p * 2 * NF
        zp = zx.at[:, cols(p)]
        if p < PIECES - 1:
            @pl.loop(0, 2 * NF)
            def _(i):
                for at, fn in hooks:
                    pl.when(mid & (i == at))(fn)
                s = gu_wait(t0 + i)
                m, c = lax.rem(i, 2), ft(lax.div(i, 2))
                if p == 0:
                    acc[m, :, c] = dot(zp[...], kbuf[s])
                else:
                    acc[m, :, c] += dot(zp[...], kbuf[s])
                gu_next(t0 + i)
        else:
            @pl.loop(0, NF)
            def _(i):
                for at, fn in hooks:
                    pl.when(mid & (i == at))(fn)
                c = ft(i)
                s = gu_wait(t0 + 2 * i)
                g = acc[0, :, c] + dot(zp[...], kbuf[s])
                acc[0, :, c] = g * jax.nn.sigmoid(g)
                gu_next(t0 + 2 * i)
                s = gu_wait(t0 + 2 * i + 1)
                hbuf[:, c] = (acc[0, :, c] * (acc[1, :, c] + dot(zp[...], kbuf[s]))).astype(BF16)
                gu_next(t0 + 2 * i + 1)

    def dn_piece(f, p):
        ox = za if f == 0 else zb
        t = f * PIECES + p
        dn_copy(t).wait()
        ox[:, cols(p)] = dot(hbuf[...], dbuf[lax.rem(t, DBUF)]).astype(BF16)

        @pl.when(t + DBUF < 2 * PIECES)
        def _():
            dn_copy(t + DBUF).start()

    def out_far(f, p, start):
        ox = za if f == 0 else zb
        ss = s_outa if f == 0 else s_outb

        def to(kk, dev):
            return send(ox.at[rows(kk), cols(p)], rof.at[f, rows(q), cols(p)], ss.at[kk, p],
                        r_rof.at[f, q, p], dev)

        @pl.when(mid)
        def _():
            c = to(1 - k, partner)
            if start:
                c.start()
                rof[f, rows(q), cols(p)] = ox[rows(k), cols(p)]
            else:
                c.wait_send()

        @pl.when(end)
        def _():
            for kk in range(2):
                c = to(kk, other + kk)
                c.start() if start else c.wait_send()

    def out_near_a(p):
        return [send(za.at[rows(2 + j), cols(p)], ro.at[rows(q), cols(p)], s_outa.at[2 + j, p],
                     r_ro.at[q, p], other + j) for j in range(2)]

    def out_near_b(p):
        return send(zb.at[rows(3 - k), cols(p)], ro.at[rows(q), cols(p)], s_outb.at[2, p], r_ro.at[q, p], partner)

    def send_part(f, p):
        dev = relay if f == 0 else far_end
        return send(xf.at[f, :, cols(p)], part.at[:, cols(p)], s_part.at[f, p], r_part.at[p], dev)

    def combine_piece(f, p):
        for qq in (qp, qo, qo + 1):
            recv(rof.at[f, rows(qq), cols(p)], r_rof.at[f, qq, p])
        xf[f, :, cols(p)] = dot(wt[1 + f], rof[f, :, cols(p)]).astype(BF16)
        send_part(f, p).start()

    for p in range(PIECES):
        @pl.when(mid)
        def _(p=p):
            relay_piece(0, p)
            if p + 2 < PIECES:
                for c in own_copies(p + 2)[1]:
                    c.start()
            if p == 1:
                pl.semaphore_signal(go, inc=1, device_id=(dp, far_end), device_id_type=MESH)

        if p == 2:
            @pl.when(end)
            def _():
                pl.semaphore_wait(go, 1)
                for pp in range(PIECES):
                    send_x(pp).start()

        await_z(0, p)
        gu_piece(0, p)

    @pl.loop(0, PIECES)
    def _(p):
        @pl.when(mid & (p == 0))
        def _():
            relay_piece(1, 0)

        @pl.when(mid & (p == 3))
        def _():
            relay_piece(1, 1)

        dn_piece(0, p)
        out_far(0, p, True)

    for p in range(PIECES):
        for c in out_near_a(p):
            c.start()

    hooks = {1: ((3, 0),), 2: ((2, 1),), 3: ((0, 2), (1, 3))}
    for p in range(PIECES):
        @pl.when(mid)
        def _(p=p):
            if p + 1 >= 2 and p + 1 < PIECES:
                relay_piece(1, p + 1)

        await_z(1, p)
        gu_piece(1, p, [(at, functools.partial(combine_piece, 0, pp)) for at, pp in hooks.get(p, ())])

    @pl.loop(0, PIECES)
    def _(p):
        dn_piece(1, p)
        out_far(1, p, True)
        out_near_b(p).start()
        ro[rows(q), cols(p)] = zb[rows(2 + k), cols(p)]

    @pl.when(mid)
    def _():
        for p in range(PIECES):
            combine_piece(1, p)

    send_meta.wait_send()
    for p in range(PIECES):
        send_x(p).wait_send()
    ycopy = [pltpu.make_async_copy(xv.at[:, cols(p)], y_hbm.at[:, cols(p)], ysem.at[p]) for p in range(PIECES)]
    for p in range(PIECES):
        recv(ro.at[rows(qp), cols(p)], r_ro.at[qp, p])
        for j in range(2):
            recv(ro.at[rows(qo + j), cols(p)], r_ro.at[qo + j, p])
        recv(part.at[:, cols(p)], r_part.at[p])
        xv[:, cols(p)] = (dot(wt[0], ro[:, cols(p)]) + part[:, cols(p)].astype(F32)).astype(BF16)
        ycopy[p].start()

    for p in range(PIECES):
        a, b = own_copies(p)
        for c in (a, *b, *out_near_a(p), out_near_b(p)):
            c.wait_send()
        for f in range(2):
            out_far(f, p, False)

    @pl.when(mid)
    def _():
        for p in range(PIECES):
            for f in range(2):
                for c in relay_copies(f, p):
                    c.wait_send()
                send_part(f, p).wait_send()

    for c in ycopy:
        c.wait()


def solution(mesh):
    def step(x, expert, slot, gate, w_gate, w_up, w_down):
        tokens, depth = x.shape[2:]
        ff = w_gate.shape[2]
        top = expert.shape[3]
        slots = 5 * tokens * top // (4 * 8)
        half = 4 * slots
        dma = pltpu.SemaphoreType.DMA
        vmem = pltpu.VMEM
        hbm = pl.BlockSpec(memory_space=pl.ANY)
        y = pl.pallas_call(
            functools.partial(kernel, slots),
            out_shape=jax.ShapeDtypeStruct((tokens, depth), BF16),
            in_specs=[pl.BlockSpec(memory_space=pltpu.VMEM)] * 3 + [hbm] * 4,
            out_specs=hbm,
            scratch_shapes=[
                vmem((8, tokens), F32),
                vmem((tokens, depth), BF16),
                vmem((2, tokens, depth), BF16),
                vmem((2, 8, tokens), F32),
                vmem((3, half, tokens), BF16),
                vmem((3, tokens, half), BF16),
                vmem((half, depth), BF16),
                vmem((half, depth), BF16),
                vmem((half, depth), BF16),
                vmem((2, half, depth), BF16),
                vmem((2, half, ff), F32),
                vmem((half, ff), BF16),
                vmem((half, depth), BF16),
                vmem((2, half, depth), BF16),
                vmem((tokens, depth), BF16),
                vmem((NBUF, depth // PIECES, ff // 2), BF16),
                vmem((DBUF, ff, depth // PIECES), BF16),
                dma((PIECES,)), dma((NBUF,)), dma((DBUF,)), dma((PIECES,)),
                pltpu.SemaphoreType.REGULAR,
                dma, dma((PIECES,)), dma((3, PIECES)), dma((2, 3, PIECES)),
                dma((4, PIECES)), dma((3, PIECES)), dma((2, PIECES)),
                dma((2,)), dma((2, PIECES)), dma((2, PIECES)), dma((PIECES,)),
                dma((2, PIECES)), dma((2, PIECES)), dma((2, 4, PIECES)), dma((4, PIECES)), dma((PIECES,)),
            ],
            compiler_params=pltpu.CompilerParams(
                collective_id=0, has_side_effects=True, vmem_limit_bytes=67043328),
        )(*(v.reshape(tokens, top).T for v in (expert, slot, gate)),
          x.reshape(tokens, depth), w_gate[0], w_up[0], w_down[0])
        return y.reshape(x.shape)

    tok = P("dp", "ep")
    return jax.shard_map(step, mesh=mesh, in_specs=(tok,) * 4 + (P("ep"),) * 3, out_specs=tok, check_vma=False)
```

```python
import functools

import jax
import jax.numpy as jnp
from jax import lax
from jax.experimental import pallas as pl
from jax.experimental.pallas import tpu as pltpu
from jax.sharding import PartitionSpec as P

MESH = pl.DeviceIdType.MESH
F32, BF16 = jnp.float32, jnp.bfloat16
PIECES = 4
NBUF = 4
DBUF = 2


def kernel(slots, expert, slot, gate, x_hbm, wg, wu, wd, y_hbm,
           meta, xv, xf, mf, oh, wt, zz, stage, stagef, acc, hbuf, ro, rof,
           part, kbuf, dbuf,
           xsem, ksem, dsem, ysem, go,
           s_meta, s_x, s_own, s_rel, s_far, s_out, s_part,
           r_meta, r_x, r_z, r_zp, r_zn, r_rof, r_ro, r_part):
    S = slots
    T, D = xv.shape
    FF = hbuf.shape[1]
    KT, FT = kbuf.shape[1:]
    NT = dbuf.shape[2]
    C = D // PIECES
    HALF = 4 * S
    NF = FF // FT
    GU = 2 * NF * PIECES

    dp = lax.axis_index("dp")
    me = lax.axis_index("ep")
    z = lax.div(me, 2)
    k = lax.rem(me, 2)
    h = lax.div(me, 4)
    q = lax.rem(me, 4)
    side = lax.rem(z + h + 1, 2)
    mid = side == 0
    end = side == 1
    partner = 2 * z + 1 - k
    qp = partner - 4 * h
    other = 2 + 8 * h - 2 * z
    qo = other - 4 * h
    relay = 4 - 2 * h + k
    far_end = 6 - 6 * h + k
    base = h * HALF
    own = 1 - side

    def rows(i):
        return pl.ds(pl.multiple_of(i * S, 16), S)

    def cols(p):
        return pl.ds(pl.multiple_of(p * C, 128), C)

    def send(src, dst, ssem, rsem, dev):
        return pltpu.make_async_remote_copy(
            src_ref=src, dst_ref=dst, send_sem=ssem, recv_sem=rsem,
            device_id=(dp, dev), device_id_type=MESH)

    def recv(dst, rsem):
        pltpu.make_async_remote_copy(
            src_ref=dst, dst_ref=dst, send_sem=rsem, recv_sem=rsem,
            device_id=(dp, partner), device_id_type=MESH).wait_recv()

    def gu_copy(t, w, m):
        t = lax.rem(t, GU)
        r = pl.ds(pl.multiple_of(lax.div(t, 2 * NF) * KT, 128), KT)
        c = pl.ds(pl.multiple_of(lax.div(lax.rem(t, 2 * NF), 2) * FT, 128), FT)
        return w.at[r, c]

    def gu_start(t):
        s = lax.rem(t, NBUF)

        @pl.when(lax.rem(t, 2) == 0)
        def _():
            pltpu.make_async_copy(gu_copy(t, wg, 0), kbuf.at[s], ksem.at[s]).start()

        @pl.when(lax.rem(t, 2) == 1)
        def _():
            pltpu.make_async_copy(gu_copy(t, wu, 1), kbuf.at[s], ksem.at[s]).start()

    def gu_wait(t):
        s = lax.rem(t, NBUF)
        pltpu.make_async_copy(gu_copy(t, wg, 0), kbuf.at[s], ksem.at[s]).wait()
        return s

    def dn_copy(t):
        s = lax.rem(t, DBUF)
        tile = pl.ds(pl.multiple_of(lax.rem(t, PIECES) * NT, 128), NT)
        return pltpu.make_async_copy(wd.at[:, tile], dbuf.at[s], dsem.at[s])

    xload = [pltpu.make_async_copy(x_hbm.at[:, cols(p)], xv.at[:, cols(p)], xsem.at[p])
             for p in range(PIECES)]
    for c in xload:
        c.start()
    for t in range(NBUF):
        gu_start(jnp.int32(t))
    for t in range(DBUF):
        dn_copy(jnp.int32(t)).start()

    barrier = pltpu.get_barrier_semaphore()

    def greet(d):
        pl.semaphore_signal(barrier, inc=1, device_id=(dp, d), device_id_type=MESH)

    for d in (partner, other, other + 1, relay):
        greet(d)
    pl.when(mid)(lambda: greet(far_end))

    def onehot(m):
        idx = m[...].astype(jnp.int32) - base
        r = lax.broadcasted_iota(jnp.int32, (HALF, T), 0)
        hit = (r == idx[0:1, :]) | (r == idx[1:2, :])
        return jnp.where(hit, 1.0, 0.0).astype(BF16)

    def weights_of(m):
        mt = jnp.transpose(jnp.concatenate([m[...], jnp.zeros((120, T), F32)], axis=0))
        idx = mt.astype(jnp.int32) - base
        r = lax.broadcasted_iota(jnp.int32, (T, HALF), 1)
        w = jnp.where(r == idx[:, 0:1], mt[:, 2:3], 0.0)
        w = jnp.where(r == idx[:, 1:2], mt[:, 3:4], w)
        return w.astype(BF16)

    def dot(a, b):
        return jnp.dot(a, b, preferred_element_type=F32)

    meta[...] = jnp.zeros_like(meta)
    meta[0:2, :] = jnp.where(slot[...] < S, expert[...] * S + slot[...], -100000).astype(F32)
    meta[2:4, :] = gate[...]
    oh[0] = onehot(meta)
    pl.semaphore_wait(barrier, 5 - side)

    send_meta = send(meta, mf.at[side], s_meta, r_meta.at[side], relay)

    def send_x(p):
        return send(xv.at[:, cols(p)], xf.at[side, :, cols(p)], s_x.at[p], r_x.at[side, p], relay)

    def own_copies(p):
        a = send(stage.at[rows(qp), cols(p)], zz.at[own, rows(2 + k), cols(p)], s_own.at[0, p], r_zp.at[p], partner)
        b = [send(stage.at[rows(qo + j), cols(p)], zz.at[own, rows(2 + k), cols(p)], s_own.at[1 + j, p],
                  r_zn.at[k, p], other + j) for j in range(2)]
        return a, b

    send_meta.start()
    for p in range(PIECES):
        xload[p].wait()

        @pl.when(mid)
        def _(p=p):
            send_x(p).start()

    for p in range(PIECES):
        stage[:, cols(p)] = dot(oh[0], xv[:, cols(p)]).astype(BF16)
        a, b = own_copies(p)
        a.start()

        @pl.when(end)
        def _(b=b):
            for c in b:
                c.start()

        zz[own, rows(2 + k), cols(p)] = stage[rows(q), cols(p)]

    def relay_copies(f, p):
        return [send(stagef.at[f, rows(qd), cols(p)], zz.at[f, rows(k), cols(p)], s_rel.at[f, j, p],
                     r_z.at[f, k, p], dev)
                for j, (qd, dev) in enumerate(((qp, partner), (qo, other), (qo + 1, other + 1)))]

    def relay_head(f):
        recv(mf.at[f], r_meta.at[f])
        oh[1 + f] = onehot(mf.at[f])

    def relay_piece(f, p):
        recv(xf.at[f, :, cols(p)], r_x.at[f, p])
        stagef[f, :, cols(p)] = dot(oh[1 + f], xf[f, :, cols(p)]).astype(BF16)
        for c in relay_copies(f, p):
            c.start()
        zz[f, rows(k), cols(p)] = stagef[f, rows(q), cols(p)]

    def await_z(f, p):
        recv(zz.at[f, rows(1 - k), cols(p)], r_z.at[f, 1 - k, p])

        @pl.when(end)
        def _():
            recv(zz.at[f, rows(k), cols(p)], r_z.at[f, k, p])

        @pl.when(own == f)
        def _():
            recv(zz.at[f, rows(3 - k), cols(p)], r_zp.at[p])

        @pl.when(own != f)
        def _():
            for j in range(2):
                recv(zz.at[f, rows(2 + j), cols(p)], r_zn.at[j, p])

    def ft(c):
        return pl.ds(pl.multiple_of(c * FT, 128), FT)

    def gu_next(t):
        @pl.when(t + NBUF < 2 * GU)
        def _():
            gu_start(t + NBUF)

    def gu_piece(f, p):
        t0 = f * GU + p * 2 * NF
        zp = zz.at[f, :, cols(p)]

        @pl.loop(0, NF)
        def _(i):
            if p == 2:
                @pl.when(end & (f == 0) & (i == 1))
                def _():
                    for pp in range(1, PIECES):
                        send_x(pp).start()

            c = ft(i)
            t = t0 + 2 * i
            sg, su = gu_wait(t), gu_wait(t + 1)
            g = dot(zp[...], kbuf[sg])
            if p == 0:
                acc[0, :, c] = g
                acc[1, :, c] = dot(zp[...], kbuf[su])
            elif p < PIECES - 1:
                acc[0, :, c] += g
                acc[1, :, c] += dot(zp[...], kbuf[su])
            else:
                g = acc[0, :, c] + g
                acc[0, :, c] = g * jax.nn.sigmoid(g)
                hbuf[:, c] = (acc[0, :, c] * (acc[1, :, c] + dot(zp[...], kbuf[su]))).astype(BF16)
            gu_next(t)
            gu_next(t + 1)

    def dn_piece(f, p):
        t = f * PIECES + p
        dn_copy(t).wait()
        zz[f, :, cols(p)] = dot(hbuf[...], dbuf[lax.rem(t, DBUF)]).astype(BF16)

        @pl.when(t + DBUF < 2 * PIECES)
        def _():
            dn_copy(t + DBUF).start()

    def out_far(f, p, start):
        def to(kk, dev):
            return send(zz.at[f, rows(kk), cols(p)], rof.at[f, rows(q), cols(p)], s_far.at[f, kk, p],
                        r_rof.at[f, q, p], dev)

        @pl.when(mid)
        def _():
            c = to(1 - k, partner)
            if start:
                c.start()
                rof[f, rows(q), cols(p)] = zz[f, rows(k), cols(p)]
            else:
                c.wait_send()

        @pl.when(end)
        def _():
            for kk in range(2):
                c = to(kk, other + kk)
                c.start() if start else c.wait_send()

    def out_chip(p):
        return send(zz.at[own, rows(3 - k), cols(p)], ro.at[rows(q), cols(p)], s_out.at[0, p], r_ro.at[q, p], partner)

    def out_other(p):
        return [send(zz.at[1 - own, rows(2 + j), cols(p)], ro.at[rows(q), cols(p)], s_out.at[1 + j, p],
                     r_ro.at[q, p], other + j) for j in range(2)]

    def send_part(f, p):
        dev = relay if f == 0 else far_end
        return send(xf.at[f, :, cols(p)], part.at[:, cols(p)], s_part.at[f, p], r_part.at[p], dev)

    def combine_piece(f, p):
        for qq in (qp, qo, qo + 1):
            recv(rof.at[f, rows(qq), cols(p)], r_rof.at[f, qq, p])
        xf[f, :, cols(p)] = dot(wt[1 + f], rof[f, :, cols(p)]).astype(BF16)
        send_part(f, p).start()

    pl.when(mid)(lambda: relay_head(0))

    @pl.loop(0, 2)
    def _(f):
        for p in range(PIECES):
            @pl.when(mid & ((f == 0) | (p < 2)))
            def _(p=p):
                relay_piece(f, p + 2 * f)

            if p == 1:
                @pl.when(mid & (f == 1))
                def _():
                    for pp in range(PIECES):
                        for c in out_other(pp):
                            c.start()

            if p == 2:
                @pl.when(mid & (f == 0))
                def _():
                    pl.semaphore_signal(go, inc=1, device_id=(dp, far_end), device_id_type=MESH)

                @pl.when(end & (f == 0))
                def _():
                    pl.semaphore_wait(go, 1)
                    send_x(0).start()

            if p == 3:
                @pl.when(mid & (f == 0))
                def _():
                    for pp in range(PIECES):
                        for c in own_copies(pp)[1]:
                            c.start()

                @pl.when(mid)
                def _():
                    wt[1 + f] = weights_of(mf.at[f])

            if p > 0:
                @pl.when(mid & (f == 1))
                def _(p=p):
                    combine_piece(0, p - 1)

            await_z(f, p)
            gu_piece(f, p)

        @pl.when(mid & (f == 1))
        def _():
            combine_piece(0, PIECES - 1)

        @pl.loop(0, PIECES)
        def _(p):
            @pl.when(mid & (f == 0) & (p == 0))
            def _():
                relay_head(1)
                relay_piece(1, 0)

            @pl.when(mid & (f == 0) & (p == 2))
            def _():
                relay_piece(1, 1)

            dn_piece(f, p)
            out_far(f, p, True)

            @pl.when(f == own)
            def _():
                out_chip(p).start()
                ro[rows(q), cols(p)] = zz[f, rows(2 + k), cols(p)]

        @pl.when(end & (f == 1))
        def _():
            for p in range(PIECES):
                for c in out_other(p):
                    c.start()

    @pl.when(mid)
    def _():
        for p in range(PIECES):
            combine_piece(1, p)

    wt[0] = weights_of(meta)
    send_meta.wait_send()
    for p in range(PIECES):
        send_x(p).wait_send()
    ycopy = [pltpu.make_async_copy(xv.at[:, cols(p)], y_hbm.at[:, cols(p)], ysem.at[p]) for p in range(PIECES)]
    for p in range(PIECES):
        recv(ro.at[rows(qp), cols(p)], r_ro.at[qp, p])
        for j in range(2):
            recv(ro.at[rows(qo + j), cols(p)], r_ro.at[qo + j, p])
        recv(part.at[:, cols(p)], r_part.at[p])
        xv[:, cols(p)] = (dot(wt[0], ro[:, cols(p)]) + part[:, cols(p)].astype(F32)).astype(BF16)
        ycopy[p].start()

    for p in range(PIECES):
        a, b = own_copies(p)
        for c in (a, *b, out_chip(p), *out_other(p)):
            c.wait_send()
        for f in range(2):
            out_far(f, p, False)

    @pl.when(mid)
    def _():
        for p in range(PIECES):
            for f in range(2):
                for c in relay_copies(f, p):
                    c.wait_send()
                send_part(f, p).wait_send()

    for c in ycopy:
        c.wait()


def solution(mesh):
    def step(x, expert, slot, gate, w_gate, w_up, w_down):
        tokens, depth = x.shape[2:]
        ff = w_gate.shape[2]
        top = expert.shape[3]
        slots = 5 * tokens * top // (4 * 8)
        half = 4 * slots
        dma = pltpu.SemaphoreType.DMA
        vmem = pltpu.VMEM
        hbm = pl.BlockSpec(memory_space=pl.ANY)
        y = pl.pallas_call(
            functools.partial(kernel, slots),
            out_shape=jax.ShapeDtypeStruct((tokens, depth), BF16),
            in_specs=[pl.BlockSpec(memory_space=pltpu.VMEM)] * 3 + [hbm] * 4,
            out_specs=hbm,
            scratch_shapes=[
                vmem((8, tokens), F32),
                vmem((tokens, depth), BF16),
                vmem((2, tokens, depth), BF16),
                vmem((2, 8, tokens), F32),
                vmem((3, half, tokens), BF16),
                vmem((3, tokens, half), BF16),
                vmem((2, half, depth), BF16),
                vmem((half, depth), BF16),
                vmem((2, half, depth), BF16),
                vmem((2, half, ff), F32),
                vmem((half, ff), BF16),
                vmem((half, depth), BF16),
                vmem((2, half, depth), BF16),
                vmem((tokens, depth), BF16),
                vmem((NBUF, depth // PIECES, ff // 2), BF16),
                vmem((DBUF, ff, depth // PIECES), BF16),
                dma((PIECES,)), dma((NBUF,)), dma((DBUF,)), dma((PIECES,)),
                pltpu.SemaphoreType.REGULAR,
                dma, dma((PIECES,)), dma((3, PIECES)), dma((2, 3, PIECES)),
                dma((2, 2, PIECES)), dma((3, PIECES)), dma((2, PIECES)),
                dma((2,)), dma((2, PIECES)), dma((2, 2, PIECES)), dma((PIECES,)), dma((2, PIECES)),
                dma((2, 4, PIECES)), dma((4, PIECES)), dma((PIECES,)),
            ],
            compiler_params=pltpu.CompilerParams(
                collective_id=0, has_side_effects=True, vmem_limit_bytes=67043328),
        )(*(v.reshape(tokens, top).T for v in (expert, slot, gate)),
          x.reshape(tokens, depth), w_gate[0], w_up[0], w_down[0])
        return y.reshape(x.shape)

    tok = P("dp", "ep")
    return jax.shard_map(step, mesh=mesh, in_specs=(tok,) * 4 + (P("ep"),) * 3, out_specs=tok, check_vma=False)
```

```python
import functools

import jax
import jax.numpy as jnp
from jax import lax
from jax.experimental import pallas as pl
from jax.experimental.pallas import tpu as pltpu
from jax.sharding import PartitionSpec as P

MESH = pl.DeviceIdType.MESH
F32, BF16 = jnp.float32, jnp.bfloat16
PIECES = 4
ROWS = 176
NBUF = 4
DBUF = 2


def kernel(slots, groups, expert, slot, gate, x_hbm, wg, wu, wd, y_hbm, most,
           meta, mc, xv, xc, xf, mf, oc, oh, wt, counts, zz, stage, stagef, acc, hbuf, ro, rof,
           part, kbuf, dbuf,
           xsem, ksem, dsem, ysem, go,
           s_meta, s_x, s_own, s_rel, s_far, s_out, s_part,
           r_meta, r_x, r_z, r_zp, r_zn, r_rof, r_ro, r_part, s_count, r_count):
    S = slots
    T, D = xv.shape
    FF = hbuf.shape[1]
    KT, FT = kbuf.shape[1:]
    NT = dbuf.shape[2]
    C = D // PIECES
    HALF = 4 * S
    NF = FF // FT
    GU = 2 * NF * PIECES

    dp = lax.axis_index("dp")
    me = lax.axis_index("ep")
    z = lax.div(me, 2)
    k = lax.rem(me, 2)
    h = lax.div(me, 4)
    q = lax.rem(me, 4)
    side = lax.rem(z + h + 1, 2)
    mid = side == 0
    end = side == 1
    partner = 2 * z + 1 - k
    qp = partner - 4 * h
    other = 2 + 8 * h - 2 * z
    qo = other - 4 * h
    relay = 4 - 2 * h + k
    far_end = 6 - 6 * h + k
    base = h * HALF
    block = side * 2 + (1 - side) * (2 + k)

    def rows(i):
        return pl.ds(pl.multiple_of(i * S, 16), S)

    def cols(p):
        return pl.ds(pl.multiple_of(p * C, 128), C)

    def send(src, dst, ssem, rsem, dev):
        return pltpu.make_async_remote_copy(
            src_ref=src, dst_ref=dst, send_sem=ssem, recv_sem=rsem,
            device_id=(dp, dev), device_id_type=MESH)

    def recv(dst, rsem):
        pltpu.make_async_remote_copy(
            src_ref=dst, dst_ref=dst, send_sem=rsem, recv_sem=rsem,
            device_id=(dp, partner), device_id_type=MESH).wait_recv()

    def gu_copy(t, w, m):
        t = lax.rem(t, GU)
        r = pl.ds(pl.multiple_of(lax.div(t, 2 * NF) * KT, 128), KT)
        c = pl.ds(pl.multiple_of(lax.div(lax.rem(t, 2 * NF), 2) * FT, 128), FT)
        return w.at[r, c]

    def gu_start(t):
        s = lax.rem(t, NBUF)

        @pl.when(lax.rem(t, 2) == 0)
        def _():
            pltpu.make_async_copy(gu_copy(t, wg, 0), kbuf.at[s], ksem.at[s]).start()

        @pl.when(lax.rem(t, 2) == 1)
        def _():
            pltpu.make_async_copy(gu_copy(t, wu, 1), kbuf.at[s], ksem.at[s]).start()

    def gu_wait(t):
        s = lax.rem(t, NBUF)
        pltpu.make_async_copy(gu_copy(t, wg, 0), kbuf.at[s], ksem.at[s]).wait()
        return s

    def dn_copy(t):
        s = lax.rem(t, DBUF)
        tile = pl.ds(pl.multiple_of(lax.rem(t, PIECES) * NT, 128), NT)
        return pltpu.make_async_copy(wd.at[:, tile], dbuf.at[s], dsem.at[s])

    xload = [pltpu.make_async_copy(x_hbm.at[:, cols(p)], xv.at[:, cols(p)], xsem.at[p])
             for p in range(PIECES)]
    for c in xload:
        c.start()
    for t in range(NBUF):
        gu_start(jnp.int32(t))
    for t in range(DBUF):
        dn_copy(jnp.int32(t)).start()

    barrier = pltpu.get_barrier_semaphore()

    def greet(d):
        pl.semaphore_signal(barrier, inc=1, device_id=d, device_id_type=MESH)

    peers = [(dp, lax.rem(me + d, 8)) for d in range(1, 8)]
    peers += [(lax.rem(dp + d, groups), me) for d in range(1, groups)]
    for d in peers:
        greet(d)

    def onehot(m, first):
        idx = m[...].astype(jnp.int32) - first
        r = lax.broadcasted_iota(jnp.int32, (HALF, T), 0)
        hit = (r == idx[0:1, :]) | (r == idx[1:2, :])
        return jnp.where(hit, 1.0, 0.0).astype(BF16)

    def by_token(m):
        return jnp.transpose(jnp.concatenate([m[...], jnp.zeros((120, T), F32)], axis=0))

    def weights_of(mt, first):
        idx = mt.astype(jnp.int32) - first
        r = lax.broadcasted_iota(jnp.int32, (T, HALF), 1)
        w = jnp.where(r == idx[:, 0:1], mt[:, 2:3], 0.0)
        w = jnp.where(r == idx[:, 1:2], mt[:, 3:4], w)
        return w.astype(BF16)

    def dot(a, b):
        return jnp.dot(a, b, preferred_element_type=F32)

    meta[...] = jnp.zeros_like(meta)
    meta[0:2, :] = jnp.where(slot[...] < S, expert[...] * S + slot[...], -100000).astype(F32)
    meta[2:4, :] = gate[...]
    oh[0] = onehot(meta, base)

    far = expert[...] - 4 * (1 - h)
    there = (far >= 0) & (far < 4) & (slot[...] < S)
    mc[...] = jnp.zeros_like(mc)
    mc[0:2, :] = jnp.where(there, far, -4).astype(F32)
    mc[2:4, :] = jnp.where(there, slot[...], 0).astype(F32)
    mc[4:6, :] = gate[...]
    cross = jnp.max(jnp.where(there, 1.0, 0.0), axis=0, keepdims=True)
    before = lax.broadcasted_iota(jnp.int32, (T, T), 0) < lax.broadcasted_iota(jnp.int32, (T, T), 1)
    rank = dot(jnp.broadcast_to(cross, (8, T)).astype(BF16), jnp.where(before, 1.0, 0.0).astype(BF16))[0:1, :]
    rank = jnp.where(cross > 0, rank, -1.0)
    meta[4:5, :] = rank
    oc[...] = jnp.where(lax.broadcasted_iota(jnp.int32, (T, T), 0) == rank.astype(jnp.int32), 1.0, 0.0).astype(BF16)
    m = lax.dot_general(mc[...].astype(BF16), oc[...], (((1,), (1,)), ((), ())), preferred_element_type=F32)
    mc[0:2, :] = m[0:2, :] * S + m[2:4, :]
    mc[2:4, :] = m[4:6, :]
    counts[0] = jnp.broadcast_to(jnp.sum(cross, axis=1, keepdims=True), counts.shape[1:])
    pl.semaphore_wait(barrier, len(peers))

    send_meta = send(mc, mf.at[side], s_meta, r_meta.at[side], relay)

    def send_x(p):
        return send(xc.at[:, cols(p)], xf.at[side, :, cols(p)], s_x.at[p], r_x.at[side, p], relay)

    def own_copy(p):
        return send(stage.at[rows(qp), cols(p)], zz.at[1, rows(block), cols(p)], s_own.at[0, p], r_zp.at[p], partner)

    def near_copy(j, p):
        f = (1 - side) * lax.rem(k + j, 2)
        r = (1 - side) * 3 + side * (2 + k)
        return send(stage.at[rows(qo + j), cols(p)], zz.at[f, rows(r), cols(p)], s_own.at[1 + j, p],
                    r_zn.at[k, p], other + j)

    send_meta.start()
    for p in range(PIECES):
        xload[p].wait()
        xc[:, cols(p)] = dot(oc[0:ROWS, :], xv[:, cols(p)]).astype(BF16)

        @pl.when(mid)
        def _(p=p):
            send_x(p).start()

    for p in range(PIECES):
        stage[:, cols(p)] = dot(oh[0], xv[:, cols(p)]).astype(BF16)
        own_copy(p).start()

        @pl.when(end)
        def _(p=p):
            for j in range(2):
                near_copy(j, p).start()

        zz[1 - side, rows(block), cols(p)] = stage[rows(q), cols(p)]

    def count_copy(d):
        if d < 8:
            return send(counts.at[0], counts.at[d], s_count.at[d], r_count.at[d], lax.rem(me + d, 8))
        return pltpu.make_async_remote_copy(
            src_ref=counts.at[11], dst_ref=counts.at[d], send_sem=s_count.at[d], recv_sem=r_count.at[d],
            device_id=(lax.rem(dp + d - 7, groups), me), device_id_type=MESH)

    for d in range(1, 8):
        count_copy(d).start()

    def count_group():
        top = counts[0]
        for d in range(1, 8):
            recv(counts.at[d], r_count.at[d])
            top = jnp.maximum(top, counts[d])
        counts[11] = top
        for d in range(8, 7 + groups):
            count_copy(d).start()

    def count_all():
        top = counts[11]
        for d in range(8, 7 + groups):
            recv(counts.at[d], r_count.at[d])
            top = jnp.maximum(top, counts[d])
        most[...] = top

    def relay_copies(f, p):
        return [send(stagef.at[f, rows(qd), cols(p)], zz.at[f, rows(k), cols(p)], s_rel.at[f, j, p],
                     r_z.at[f, k, p], dev)
                for j, (qd, dev) in enumerate(((qp, partner), (qo, other), (qo + 1, other + 1)))]

    def relay_head(f):
        recv(mf.at[f], r_meta.at[f])
        oh[1 + f] = onehot(mf.at[f], 0)

    def relay_piece(f, p):
        recv(xf.at[f, :, cols(p)], r_x.at[f, p])
        stagef[f, :, cols(p)] = dot(oh[1 + f, :, 0:ROWS], xf[f, :, cols(p)]).astype(BF16)
        for c in relay_copies(f, p):
            c.start()
        zz[f, rows(k), cols(p)] = stagef[f, rows(q), cols(p)]

    def await_z(f, p):
        recv(zz.at[f, rows(1 - k), cols(p)], r_z.at[f, 1 - k, p])

        @pl.when(end)
        def _():
            recv(zz.at[f, rows(k), cols(p)], r_z.at[f, k, p])

        @pl.when(mid & (f == 0))
        def _():
            for j in range(2):
                recv(zz.at[f, rows(2 + j), cols(p)], r_zn.at[j, p])

        @pl.when(mid & (f == 1))
        def _():
            recv(zz.at[f, rows(3 - k), cols(p)], r_zp.at[p])

        @pl.when(end & (f == 1))
        def _():
            recv(zz.at[f, rows(2), cols(p)], r_zp.at[p])

        @pl.when(end)
        def _():
            recv(zz.at[f, rows(3), cols(p)], r_zn.at[lax.rem(k + f, 2), p])

    def ft(c):
        return pl.ds(pl.multiple_of(c * FT, 128), FT)

    def gu_next(t):
        @pl.when(t + NBUF < 2 * GU)
        def _():
            gu_start(t + NBUF)

    def gu_piece(f, p):
        t0 = f * GU + p * 2 * NF
        zp = zz.at[f, :, cols(p)]

        @pl.loop(0, NF)
        def _(i):
            c = ft(i)
            t = t0 + 2 * i
            sg, su = gu_wait(t), gu_wait(t + 1)
            g = dot(zp[...], kbuf[sg])
            if p == 0:
                acc[0, :, c] = g
                acc[1, :, c] = dot(zp[...], kbuf[su])
            elif p < PIECES - 1:
                acc[0, :, c] += g
                acc[1, :, c] += dot(zp[...], kbuf[su])
            else:
                g = acc[0, :, c] + g
                acc[0, :, c] = g * jax.nn.sigmoid(g)
                hbuf[:, c] = (acc[0, :, c] * (acc[1, :, c] + dot(zp[...], kbuf[su]))).astype(BF16)
            gu_next(t)
            gu_next(t + 1)

    def dn_piece(f, p):
        t = f * PIECES + p
        dn_copy(t).wait()
        zz[f, :, cols(p)] = dot(hbuf[...], dbuf[lax.rem(t, DBUF)]).astype(BF16)

        @pl.when(t + DBUF < 2 * PIECES)
        def _():
            dn_copy(t + DBUF).start()

    def out_far(f, p, start):
        def to(kk, dev):
            return send(zz.at[f, rows(kk), cols(p)], rof.at[f, rows(q), cols(p)], s_far.at[f, kk, p],
                        r_rof.at[f, q, p], dev)

        @pl.when(mid)
        def _():
            c = to(1 - k, partner)
            if start:
                c.start()
                rof[f, rows(q), cols(p)] = zz[f, rows(k), cols(p)]
            else:
                c.wait_send()

        @pl.when(end)
        def _():
            for kk in range(2):
                c = to(kk, other + kk)
                c.start() if start else c.wait_send()

    def out_chip(p):
        r = side * 2 + (1 - side) * (3 - k)
        return send(zz.at[1, rows(r), cols(p)], ro.at[rows(q), cols(p)], s_out.at[0, p], r_ro.at[q, p], partner)

    def out_other(j, p):
        f = side * lax.rem(k + j, 2)
        r = side * 3 + (1 - side) * (2 + j)
        return send(zz.at[f, rows(r), cols(p)], ro.at[rows(q), cols(p)], s_out.at[1 + j, p],
                    r_ro.at[q, p], other + j)

    def send_part(f, p):
        dev = relay if f == 0 else far_end
        return send(xf.at[f, :, cols(p)], part.at[:, cols(p)], s_part.at[f, p], r_part.at[p], dev)

    def combine_piece(f, p):
        for qq in (qp, qo, qo + 1):
            recv(rof.at[f, rows(qq), cols(p)], r_rof.at[f, qq, p])
        xf[f, :, cols(p)] = dot(wt[1 + f, 0:ROWS, :], rof[f, :, cols(p)]).astype(BF16)
        send_part(f, p).start()

    pl.when(mid)(lambda: relay_head(0))

    @pl.loop(0, 2)
    def _(f):
        for p in range(PIECES):
            if p < 3:
                @pl.when(mid & ((f == 0) | (p < 2)))
                def _(p=p):
                    early = min(p, 1)
                    relay_piece(f, (p + early) * (1 - f) + (p + 2) * f)
                    pl.when(f == 0)(near_copy(k, p + early).start)

            if p < 2:
                pl.when(mid & (f == 1))(near_copy(1 - k, p + 2).start)

            if p == 1:
                @pl.when(mid & (f == 0))
                def _():
                    pl.semaphore_signal(go, inc=1, device_id=(dp, far_end), device_id_type=MESH)

                @pl.when(end & (f == 0))
                def _():
                    pl.semaphore_wait(go, 1)
                    for pp in range(PIECES):
                        send_x(pp).start()

                @pl.when(mid & (f == 1))
                def _():
                    wt[1] = weights_of(by_token(mf.at[0]), 0)

            if p == 2:
                @pl.when(mid & (f == 1))
                def _():
                    for pp in range(PIECES):
                        for j in range(2):
                            out_other(j, pp).start()

            if p == 3:
                @pl.when(mid & (f == 0))
                def _():
                    for pp in range(2):
                        near_copy(1 - k, pp).start()

                @pl.when(mid & (f == 1))
                def _():
                    wt[2] = weights_of(by_token(mf.at[1]), 0)

            if p > 0:
                @pl.when(mid & (f == 1))
                def _(p=p):
                    combine_piece(0, p - 1)

            await_z(f, p)
            if p == 0:
                @pl.when(mid & (f == 0))
                def _():
                    relay_piece(0, 1)
                    near_copy(k, 1).start()

            gu_piece(f, p)

        @pl.when(mid & (f == 1))
        def _():
            combine_piece(0, 3)

        pl.when(f == 0)(count_group)

        @pl.loop(0, PIECES)
        def _(p):
            @pl.when(mid & (f == 0) & (p == 1))
            def _():
                relay_head(1)
                relay_piece(1, 0)

            @pl.when(mid & (f == 0) & (p == 3))
            def _():
                relay_piece(1, 1)

            dn_piece(f, p)
            out_far(f, p, True)

            @pl.when(f == 1)
            def _():
                out_chip(p).start()

            @pl.when(f == 1 - side)
            def _():
                ro[rows(q), cols(p)] = zz[f, rows(block), cols(p)]

        @pl.when(end)
        def _():
            for p in range(PIECES):
                out_other(lax.rem(k + f, 2), p).start()

    @pl.when(mid)
    def _():
        for p in range(PIECES):
            combine_piece(1, p)

    count_all()
    mt = by_token(meta)
    wt[0] = weights_of(mt, base)
    oc[...] = jnp.where(lax.broadcasted_iota(jnp.int32, (T, T), 1) == mt[:, 4:5].astype(jnp.int32), 1.0, 0.0).astype(BF16)
    send_meta.wait_send()
    for p in range(PIECES):
        send_x(p).wait_send()
    ycopy = [pltpu.make_async_copy(xv.at[:, cols(p)], y_hbm.at[:, cols(p)], ysem.at[p]) for p in range(PIECES)]
    for p in range(PIECES):
        recv(ro.at[rows(qp), cols(p)], r_ro.at[qp, p])
        for j in range(2):
            recv(ro.at[rows(qo + j), cols(p)], r_ro.at[qo + j, p])
        recv(part.at[:, cols(p)], r_part.at[p])
        xv[:, cols(p)] = (dot(wt[0], ro[:, cols(p)]) + dot(oc[:, 0:ROWS], part[:, cols(p)])).astype(BF16)
        ycopy[p].start()

    for p in range(PIECES):
        for c in (own_copy(p), near_copy(0, p), near_copy(1, p), out_chip(p), out_other(0, p), out_other(1, p)):
            c.wait_send()
        for f in range(2):
            out_far(f, p, False)

    @pl.when(mid)
    def _():
        for p in range(PIECES):
            for f in range(2):
                for c in relay_copies(f, p):
                    c.wait_send()
                send_part(f, p).wait_send()

    for d in range(1, 7 + groups):
        count_copy(d).wait_send()
    for c in ycopy:
        c.wait()


def solution(mesh):
    def step(x, expert, slot, gate, w_gate, w_up, w_down):
        tokens, depth = x.shape[2:]
        ff = w_gate.shape[2]
        top = expert.shape[3]
        slots = 5 * tokens * top // (4 * 8)
        half = 4 * slots
        dma = pltpu.SemaphoreType.DMA
        vmem = pltpu.VMEM
        hbm = pl.BlockSpec(memory_space=pl.ANY)
        routing = [v.reshape(tokens, top) for v in (expert, slot, gate)]
        x2, wg, wu, wd = x.reshape(tokens, depth), w_gate[0], w_up[0], w_down[0]
        groups = mesh.shape["dp"]
        y, most = pl.pallas_call(
            functools.partial(kernel, slots, groups),
            out_shape=(jax.ShapeDtypeStruct((tokens, depth), BF16), jax.ShapeDtypeStruct((8, 128), F32)),
            in_specs=[pl.BlockSpec(memory_space=pltpu.VMEM)] * 3 + [hbm] * 4,
            out_specs=(hbm, pl.BlockSpec(memory_space=pltpu.VMEM)),
            scratch_shapes=[
                vmem((8, tokens), F32),
                vmem((8, tokens), F32),
                vmem((tokens, depth), BF16),
                vmem((ROWS, depth), BF16),
                vmem((2, ROWS, depth), BF16),
                vmem((2, 8, tokens), F32),
                vmem((tokens, tokens), BF16),
                vmem((3, half, tokens), BF16),
                vmem((3, tokens, half), BF16),
                vmem((12, 8, 128), F32),
                vmem((2, half, depth), BF16),
                vmem((half, depth), BF16),
                vmem((2, half, depth), BF16),
                vmem((2, half, ff), F32),
                vmem((half, ff), BF16),
                vmem((half, depth), BF16),
                vmem((2, half, depth), BF16),
                vmem((ROWS, depth), BF16),
                vmem((NBUF, depth // PIECES, ff // 2), BF16),
                vmem((DBUF, ff, depth // PIECES), BF16),
                dma((PIECES,)), dma((NBUF,)), dma((DBUF,)), dma((PIECES,)),
                pltpu.SemaphoreType.REGULAR,
                dma, dma((PIECES,)), dma((3, PIECES)), dma((2, 3, PIECES)),
                dma((2, 2, PIECES)), dma((3, PIECES)), dma((2, PIECES)),
                dma((2,)), dma((2, PIECES)), dma((2, 2, PIECES)), dma((PIECES,)), dma((2, PIECES)),
                dma((2, 4, PIECES)), dma((4, PIECES)), dma((PIECES,)), dma((11,)), dma((11,)),
            ],
            compiler_params=pltpu.CompilerParams(
                collective_id=0, has_side_effects=True, vmem_limit_bytes=67043328),
        )(*(v.T for v in routing), x2, wg, wu, wd)

        def dot(a, b):
            return jnp.dot(a, b, preferred_element_type=F32)

        def every_slot():
            e, c, g = routing
            place = jnp.where(c < slots, e * slots + c, -1)
            hit = place[:, :, None] == jnp.arange(8 * slots)
            gates = jnp.where(hit, g.astype(BF16)[:, :, None], jnp.zeros((), BF16))
            z = dot(jnp.any(hit, axis=1).astype(BF16).T, x2).astype(BF16)
            z = lax.all_to_all(z.reshape(8, slots, depth), "ep", 0, 0).reshape(8 * slots, depth)
            u = (jax.nn.silu(dot(z, wg)) * dot(z, wu)).astype(BF16)
            out = dot(u, wd).astype(BF16).reshape(8, slots, depth)
            out = lax.all_to_all(out, "ep", 0, 0).reshape(8 * slots, depth)
            return dot(jnp.sum(gates, axis=1), out).astype(BF16)

        y = lax.cond(most[0, 0] > ROWS, every_slot, lambda: y)
        return y.reshape(x.shape)

    tok = P("dp", "ep")
    return jax.shard_map(step, mesh=mesh, in_specs=(tok,) * 4 + (P("ep"),) * 3, out_specs=tok, check_vma=False)
```

```python
import functools

import jax
import jax.numpy as jnp
from jax import lax
from jax.experimental import pallas as pl
from jax.experimental.pallas import tpu as pltpu
from jax.sharding import PartitionSpec as P

MESH = pl.DeviceIdType.MESH
F32, BF16 = jnp.float32, jnp.bfloat16
PIECES = 4
ROWS = 176
NBUF = 4
DBUF = 2


def kernel(slots, groups, expert, slot, gate, x_hbm, wg, wu, wd, y_hbm, over,
           meta, mc, xv, xc, xf, mf, oc, oh, wt, counts, zz, stage, stagef, acc, hbuf, ro, rof,
           part, kbuf, dbuf,
           xsem, ksem, dsem, ysem, go,
           s_meta, s_x, s_own, s_rel, s_far, s_out, s_part,
           r_meta, r_x, r_z, r_zp, r_zn, r_rof, r_ro, r_part, s_count, r_count):
    S = slots
    T, D = xv.shape
    FF = hbuf.shape[1]
    KT, FT = kbuf.shape[1:]
    NT = dbuf.shape[2]
    C = D // PIECES
    HALF = 4 * S
    NF = FF // FT
    GU = 2 * NF * PIECES

    dp = lax.axis_index("dp")
    me = lax.axis_index("ep")
    z = lax.div(me, 2)
    k = lax.rem(me, 2)
    h = lax.div(me, 4)
    q = lax.rem(me, 4)
    side = lax.rem(z + h + 1, 2)
    mid = side == 0
    end = side == 1
    partner = 2 * z + 1 - k
    qp = partner - 4 * h
    other = 2 + 8 * h - 2 * z
    qo = other - 4 * h
    relay = 4 - 2 * h + k
    far_end = 6 - 6 * h + k
    base = h * HALF
    block = side * 2 + (1 - side) * (2 + k)

    def rows(i):
        return pl.ds(pl.multiple_of(i * S, 16), S)

    def cols(p):
        return pl.ds(pl.multiple_of(p * C, 128), C)

    def send(src, dst, ssem, rsem, dev):
        return pltpu.make_async_remote_copy(
            src_ref=src, dst_ref=dst, send_sem=ssem, recv_sem=rsem,
            device_id=(dp, dev), device_id_type=MESH)

    def recv(dst, rsem):
        pltpu.make_async_remote_copy(
            src_ref=dst, dst_ref=dst, send_sem=rsem, recv_sem=rsem,
            device_id=(dp, partner), device_id_type=MESH).wait_recv()

    def gu_copy(t, w, m):
        t = lax.rem(t, GU)
        r = pl.ds(pl.multiple_of(lax.div(t, 2 * NF) * KT, 128), KT)
        c = pl.ds(pl.multiple_of(lax.div(lax.rem(t, 2 * NF), 2) * FT, 128), FT)
        return w.at[r, c]

    def gu_start(t):
        s = lax.rem(t, NBUF)

        @pl.when(lax.rem(t, 2) == 0)
        def _():
            pltpu.make_async_copy(gu_copy(t, wg, 0), kbuf.at[s], ksem.at[s]).start()

        @pl.when(lax.rem(t, 2) == 1)
        def _():
            pltpu.make_async_copy(gu_copy(t, wu, 1), kbuf.at[s], ksem.at[s]).start()

    def gu_wait(t):
        s = lax.rem(t, NBUF)
        pltpu.make_async_copy(gu_copy(t, wg, 0), kbuf.at[s], ksem.at[s]).wait()
        return s

    def dn_copy(t):
        s = lax.rem(t, DBUF)
        tile = pl.ds(pl.multiple_of(lax.rem(t, PIECES) * NT, 128), NT)
        return pltpu.make_async_copy(wd.at[:, tile], dbuf.at[s], dsem.at[s])

    xload = [pltpu.make_async_copy(x_hbm.at[:, cols(p)], xv.at[:, cols(p)], xsem.at[p])
             for p in range(PIECES)]
    for c in xload:
        c.start()
    for t in range(NBUF):
        gu_start(jnp.int32(t))
    for t in range(DBUF):
        dn_copy(jnp.int32(t)).start()

    barrier = pltpu.get_barrier_semaphore()

    def greet(d):
        pl.semaphore_signal(barrier, inc=1, device_id=d, device_id_type=MESH)

    peers = [(dp, d) for d in (partner, other, other + 1, relay)]
    peers += [(lax.rem(dp + d, groups), me) for d in range(1, groups)]
    for d in peers:
        greet(d)
    pl.when(mid)(lambda: greet((dp, far_end)))

    def onehot(m, first):
        idx = m[...].astype(jnp.int32) - first
        r = lax.broadcasted_iota(jnp.int32, (HALF, T), 0)
        hit = (r == idx[0:1, :]) | (r == idx[1:2, :])
        return jnp.where(hit, 1.0, 0.0).astype(BF16)

    def by_token(m):
        return jnp.transpose(jnp.concatenate([m[...], jnp.zeros((120, T), F32)], axis=0))

    def weights_of(mt, first):
        idx = mt.astype(jnp.int32) - first
        r = lax.broadcasted_iota(jnp.int32, (T, HALF), 1)
        w = jnp.where(r == idx[:, 0:1], mt[:, 2:3], 0.0)
        w = jnp.where(r == idx[:, 1:2], mt[:, 3:4], w)
        return w.astype(BF16)

    def dot(a, b):
        return jnp.dot(a, b, preferred_element_type=F32)

    meta[...] = jnp.zeros_like(meta)
    meta[0:2, :] = jnp.where(slot[...] < S, expert[...] * S + slot[...], -100000).astype(F32)
    meta[2:4, :] = gate[...]
    oh[0] = onehot(meta, base)

    far = expert[...] - 4 * (1 - h)
    there = (far >= 0) & (far < 4) & (slot[...] < S)
    mc[...] = jnp.zeros_like(mc)
    mc[0:2, :] = jnp.where(there, far, -4).astype(F32)
    mc[2:4, :] = jnp.where(there, slot[...], 0).astype(F32)
    mc[4:6, :] = gate[...]
    cross = jnp.max(jnp.where(there, 1.0, 0.0), axis=0, keepdims=True)
    before = lax.broadcasted_iota(jnp.int32, (T, T), 0) < lax.broadcasted_iota(jnp.int32, (T, T), 1)
    rank = dot(jnp.broadcast_to(cross, (8, T)).astype(BF16), jnp.where(before, 1.0, 0.0).astype(BF16))[0:1, :]
    rank = jnp.where(cross > 0, rank, -1.0)
    meta[4:5, :] = rank
    oc[...] = jnp.where(lax.broadcasted_iota(jnp.int32, (T, T), 0) == rank.astype(jnp.int32), 1.0, 0.0).astype(BF16)
    m = lax.dot_general(mc[...].astype(BF16), oc[...], (((1,), (1,)), ((), ())), preferred_element_type=F32)
    mc[0:2, :] = m[0:2, :] * S + m[2:4, :]
    mc[2:4, :] = m[4:6, :]
    counts[0] = jnp.broadcast_to(jnp.sum(cross, axis=1, keepdims=True), counts.shape[1:])
    pl.semaphore_wait(barrier, len(peers) + 1 - side)

    send_meta = send(mc, mf.at[side], s_meta, r_meta.at[side], relay)

    def send_x(p):
        return send(xc.at[:, cols(p)], xf.at[side, :, cols(p)], s_x.at[p], r_x.at[side, p], relay)

    def own_copy(p):
        return send(stage.at[rows(qp), cols(p)], zz.at[1, rows(block), cols(p)], s_own.at[0, p], r_zp.at[p], partner)

    def near_copy(j, p):
        f = (1 - side) * lax.rem(k + j, 2)
        r = (1 - side) * 3 + side * (2 + k)
        return send(stage.at[rows(qo + j), cols(p)], zz.at[f, rows(r), cols(p)], s_own.at[1 + j, p],
                    r_zn.at[k, p], other + j)

    send_meta.start()
    def pack_x(p):
        xc[:, cols(p)] = dot(oc[0:ROWS, :], xv[:, cols(p)]).astype(BF16)

    for p in range(PIECES):
        xload[p].wait()

        @pl.when(mid)
        def _(p=p):
            pack_x(p)
            send_x(p).start()

    for p in range(PIECES):
        stage[:, cols(p)] = dot(oh[0], xv[:, cols(p)]).astype(BF16)
        if p < 2:
            pl.when(mid)(near_copy(k, p).start)
        own_copy(p).start()

        @pl.when(end)
        def _(p=p):
            for j in range(2):
                near_copy(j, p).start()

        zz[1 - side, rows(block), cols(p)] = stage[rows(q), cols(p)]

    @pl.when(end)
    def _():
        for p in range(PIECES):
            pack_x(p)

    def count_copy(src, dst, i, dev):
        return pltpu.make_async_remote_copy(
            src_ref=counts.at[src], dst_ref=counts.at[dst], send_sem=s_count.at[i], recv_sem=r_count.at[dst],
            device_id=dev, device_id_type=MESH)

    count_half = [count_copy(0, 1, 1, (dp, partner)), count_copy(0, 2 + k, 2, (dp, other)),
                  count_copy(0, 2 + k, 3, (dp, other + 1))]
    count_over = [count_copy(4, 5, 4, (dp, relay)), count_copy(4, 5, 5, (dp, far_end))]
    count_dp = [count_copy(6, 6 + d, 5 + d, (lax.rem(dp + d, groups), me)) for d in range(1, groups)]
    for c in count_half:
        c.start()

    def largest(i, slots):
        top = counts[i]
        for d in slots:
            recv(counts.at[d], r_count.at[d])
            top = jnp.maximum(top, counts[d])
        return top

    def count_far():
        counts[4] = largest(0, (1, 2, 3))

        @pl.when(mid)
        def _():
            for c in count_over:
                c.start()

    def count_group():
        counts[6] = largest(4, (5,))
        for c in count_dp:
            c.start()

    def count_all():
        top = largest(6, range(7, 6 + groups))
        over[0, 0] = (jnp.max(top) > ROWS).astype(jnp.int32)

    def relay_copies(f, p):
        return [send(stagef.at[f, rows(qd), cols(p)], zz.at[f, rows(k), cols(p)], s_rel.at[f, j, p],
                     r_z.at[f, k, p], dev)
                for j, (qd, dev) in enumerate(((qp, partner), (qo, other), (qo + 1, other + 1)))]

    def relay_head(f):
        recv(mf.at[f], r_meta.at[f])
        oh[1 + f] = onehot(mf.at[f], 0)

    def relay_piece(f, p):
        recv(xf.at[f, :, cols(p)], r_x.at[f, p])
        stagef[f, :, cols(p)] = dot(oh[1 + f, :, 0:ROWS], xf[f, :, cols(p)]).astype(BF16)
        for c in relay_copies(f, p):
            c.start()
        zz[f, rows(k), cols(p)] = stagef[f, rows(q), cols(p)]

    def await_z(f, p):
        recv(zz.at[f, rows(1 - k), cols(p)], r_z.at[f, 1 - k, p])

        @pl.when(end)
        def _():
            recv(zz.at[f, rows(k), cols(p)], r_z.at[f, k, p])

        @pl.when(mid & (f == 0))
        def _():
            for j in range(2):
                recv(zz.at[f, rows(2 + j), cols(p)], r_zn.at[j, p])

        @pl.when(mid & (f == 1))
        def _():
            recv(zz.at[f, rows(3 - k), cols(p)], r_zp.at[p])

        @pl.when(end & (f == 1))
        def _():
            recv(zz.at[f, rows(2), cols(p)], r_zp.at[p])

        @pl.when(end)
        def _():
            recv(zz.at[f, rows(3), cols(p)], r_zn.at[lax.rem(k + f, 2), p])

    def ft(c):
        return pl.ds(pl.multiple_of(c * FT, 128), FT)

    def gu_next(t):
        @pl.when(t + NBUF < 2 * GU)
        def _():
            gu_start(t + NBUF)

    def gu_piece(f, p):
        t0 = f * GU + p * 2 * NF
        zp = zz.at[f, :, cols(p)]

        @pl.loop(0, NF)
        def _(i):
            c = ft(i)
            t = t0 + 2 * i
            sg, su = gu_wait(t), gu_wait(t + 1)
            g = dot(zp[...], kbuf[sg])
            if p == 0:
                acc[0, :, c] = g
                acc[1, :, c] = dot(zp[...], kbuf[su])
            elif p < PIECES - 1:
                acc[0, :, c] += g
                acc[1, :, c] += dot(zp[...], kbuf[su])
            else:
                g = acc[0, :, c] + g
                acc[0, :, c] = g * jax.nn.sigmoid(g)
                hbuf[:, c] = (acc[0, :, c] * (acc[1, :, c] + dot(zp[...], kbuf[su]))).astype(BF16)
            gu_next(t)
            gu_next(t + 1)

    def dn_piece(f, p):
        t = f * PIECES + p
        dn_copy(t).wait()
        zz[f, :, cols(p)] = dot(hbuf[...], dbuf[lax.rem(t, DBUF)]).astype(BF16)

        @pl.when(t + DBUF < 2 * PIECES)
        def _():
            dn_copy(t + DBUF).start()

    def out_far(f, p, start):
        def to(kk, dev):
            return send(zz.at[f, rows(kk), cols(p)], rof.at[f, rows(q), cols(p)], s_far.at[f, kk, p],
                        r_rof.at[f, q, p], dev)

        @pl.when(mid)
        def _():
            c = to(1 - k, partner)
            if start:
                c.start()
                rof[f, rows(q), cols(p)] = zz[f, rows(k), cols(p)]
            else:
                c.wait_send()

        @pl.when(end)
        def _():
            for kk in range(2):
                c = to(kk, other + kk)
                c.start() if start else c.wait_send()

    def out_chip(p):
        r = side * 2 + (1 - side) * (3 - k)
        return send(zz.at[1, rows(r), cols(p)], ro.at[rows(q), cols(p)], s_out.at[0, p], r_ro.at[q, p], partner)

    def out_other(j, p):
        f = side * lax.rem(k + j, 2)
        r = side * 3 + (1 - side) * (2 + j)
        return send(zz.at[f, rows(r), cols(p)], ro.at[rows(q), cols(p)], s_out.at[1 + j, p],
                    r_ro.at[q, p], other + j)

    def send_part(f, p):
        dev = relay if f == 0 else far_end
        return send(xf.at[f, :, cols(p)], part.at[:, cols(p)], s_part.at[f, p], r_part.at[p], dev)

    def combine_piece(f, p):
        for qq in (qp, qo, qo + 1):
            recv(rof.at[f, rows(qq), cols(p)], r_rof.at[f, qq, p])
        xf[f, :, cols(p)] = dot(wt[1 + f, 0:ROWS, :], rof[f, :, cols(p)]).astype(BF16)
        send_part(f, p).start()

    pl.when(mid)(lambda: relay_head(0))

    @pl.loop(0, 2)
    def _(f):
        for p in range(PIECES):
            if p < 3:
                @pl.when(mid & ((f == 0) | (p < 2)))
                def _(p=p):
                    early = min(p, 1)
                    relay_piece(f, (p + early) * (1 - f) + (p + 2) * f)
                    if p == 1:
                        pl.when(f == 0)(near_copy(k, 3).start)

            if p < 2:
                pl.when(mid & (f == 1))(near_copy(1 - k, p + 2).start)

            if p == 1:
                @pl.when(mid & (f == 0))
                def _():
                    pl.semaphore_signal(go, inc=1, device_id=(dp, far_end), device_id_type=MESH)

                @pl.when(end & (f == 0))
                def _():
                    pl.semaphore_wait(go, 1)
                    for pp in range(PIECES):
                        send_x(pp).start()

                @pl.when(mid & (f == 1))
                def _():
                    wt[1] = weights_of(by_token(mf.at[0]), 0)

            if p == 2:
                @pl.when(mid & (f == 1))
                def _():
                    for pp in range(PIECES):
                        for j in range(2):
                            out_other(j, pp).start()

            if p == 3:
                @pl.when(mid & (f == 0))
                def _():
                    for pp in range(2):
                        near_copy(1 - k, pp).start()

                @pl.when(mid & (f == 1))
                def _():
                    wt[2] = weights_of(by_token(mf.at[1]), 0)

            if p > 0:
                @pl.when(mid & (f == 1))
                def _(p=p):
                    combine_piece(0, p - 1)

            await_z(f, p)
            if p == 0:
                @pl.when(mid & (f == 0))
                def _():
                    relay_piece(0, 1)
                    near_copy(k, 2).start()

            gu_piece(f, p)

        @pl.when(mid & (f == 1))
        def _():
            combine_piece(0, 3)

        pl.when(f == 0)(count_far)
        pl.when(f == 1)(count_group)

        @pl.loop(0, PIECES)
        def _(p):
            @pl.when(mid & (f == 0) & (p == 1))
            def _():
                relay_head(1)
                relay_piece(1, 0)

            @pl.when(mid & (f == 0) & (p == 3))
            def _():
                relay_piece(1, 1)

            @pl.when(mid & (f == 1) & (p == 3))
            def _():
                combine_piece(1, 0)

            dn_piece(f, p)
            out_far(f, p, True)

            @pl.when(f == 1)
            def _():
                out_chip(p).start()

            @pl.when(f == 1 - side)
            def _():
                ro[rows(q), cols(p)] = zz[f, rows(block), cols(p)]

        @pl.when(end)
        def _():
            for p in range(PIECES):
                out_other(lax.rem(k + f, 2), p).start()

    @pl.when(mid)
    def _():
        for p in range(1, PIECES):
            combine_piece(1, p)

    count_all()
    mt = by_token(meta)
    wt[0] = weights_of(mt, base)
    oc[...] = jnp.where(lax.broadcasted_iota(jnp.int32, (T, T), 1) == mt[:, 4:5].astype(jnp.int32), 1.0, 0.0).astype(BF16)
    send_meta.wait_send()
    for p in range(PIECES):
        send_x(p).wait_send()
    ycopy = [pltpu.make_async_copy(xv.at[:, cols(p)], y_hbm.at[:, cols(p)], ysem.at[p]) for p in range(PIECES)]
    for p in range(PIECES):
        recv(ro.at[rows(qp), cols(p)], r_ro.at[qp, p])
        for j in range(2):
            recv(ro.at[rows(qo + j), cols(p)], r_ro.at[qo + j, p])
        recv(part.at[:, cols(p)], r_part.at[p])
        xv[:, cols(p)] = (dot(wt[0], ro[:, cols(p)]) + dot(oc[:, 0:ROWS], part[:, cols(p)])).astype(BF16)
        ycopy[p].start()

    for p in range(PIECES):
        for c in (own_copy(p), near_copy(0, p), near_copy(1, p), out_chip(p), out_other(0, p), out_other(1, p)):
            c.wait_send()
        for f in range(2):
            out_far(f, p, False)

    @pl.when(mid)
    def _():
        for p in range(PIECES):
            for f in range(2):
                for c in relay_copies(f, p):
                    c.wait_send()
                send_part(f, p).wait_send()

    for c in (*count_half, *count_dp):
        c.wait_send()

    @pl.when(mid)
    def _():
        for c in count_over:
            c.wait_send()

    for c in ycopy:
        c.wait()


def copy_kernel(src, dst, buf, isem, osem):
    n = buf.shape[0] // PIECES
    parts = [pl.ds(i * n, n) for i in range(PIECES)]
    load = [pltpu.make_async_copy(src.at[r], buf.at[r], isem.at[i]) for i, r in enumerate(parts)]
    save = [pltpu.make_async_copy(buf.at[r], dst.at[r], osem.at[i]) for i, r in enumerate(parts)]
    for c in load:
        c.start()
    for a, b in zip(load, save):
        a.wait()
        b.start()
    for c in save:
        c.wait()


def solution(mesh):
    def step(x, expert, slot, gate, w_gate, w_up, w_down):
        tokens, depth = x.shape[2:]
        ff = w_gate.shape[2]
        top = expert.shape[3]
        slots = 5 * tokens * top // (4 * 8)
        half = 4 * slots
        dma = pltpu.SemaphoreType.DMA
        vmem = pltpu.VMEM
        hbm = pl.BlockSpec(memory_space=pl.ANY)
        routing = [v.reshape(tokens, top) for v in (expert, slot, gate)]
        x2, wg, wu, wd = x.reshape(tokens, depth), w_gate[0], w_up[0], w_down[0]
        groups = mesh.shape["dp"]
        y, over = pl.pallas_call(
            functools.partial(kernel, slots, groups),
            out_shape=(jax.ShapeDtypeStruct((tokens, depth), BF16), jax.ShapeDtypeStruct((1, 1), jnp.int32)),
            in_specs=[pl.BlockSpec(memory_space=pltpu.VMEM)] * 3 + [hbm] * 4,
            out_specs=(hbm, pl.BlockSpec(memory_space=pltpu.SMEM)),
            scratch_shapes=[
                vmem((8, tokens), F32),
                vmem((8, tokens), F32),
                vmem((tokens, depth), BF16),
                vmem((ROWS, depth), BF16),
                vmem((2, ROWS, depth), BF16),
                vmem((2, 8, tokens), F32),
                vmem((tokens, tokens), BF16),
                vmem((3, half, tokens), BF16),
                vmem((3, tokens, half), BF16),
                vmem((12, 8, 128), F32),
                vmem((2, half, depth), BF16),
                vmem((half, depth), BF16),
                vmem((2, half, depth), BF16),
                vmem((2, half, ff), F32),
                vmem((half, ff), BF16),
                vmem((half, depth), BF16),
                vmem((2, half, depth), BF16),
                vmem((ROWS, depth), BF16),
                vmem((NBUF, depth // PIECES, ff // 2), BF16),
                vmem((DBUF, ff, depth // PIECES), BF16),
                dma((PIECES,)), dma((NBUF,)), dma((DBUF,)), dma((PIECES,)),
                pltpu.SemaphoreType.REGULAR,
                dma, dma((PIECES,)), dma((3, PIECES)), dma((2, 3, PIECES)),
                dma((2, 2, PIECES)), dma((3, PIECES)), dma((2, PIECES)),
                dma((2,)), dma((2, PIECES)), dma((2, 2, PIECES)), dma((PIECES,)), dma((2, PIECES)),
                dma((2, 4, PIECES)), dma((4, PIECES)), dma((PIECES,)), dma((11,)), dma((11,)),
            ],
            compiler_params=pltpu.CompilerParams(
                collective_id=0, has_side_effects=True, vmem_limit_bytes=67043328),
        )(*(v.T for v in routing), x2, wg, wu, wd)

        def dot(a, b):
            return jnp.dot(a, b, preferred_element_type=F32)

        def every_slot():
            e, c, g = routing
            place = jnp.where(c < slots, e * slots + c, -1)
            hit = place[:, :, None] == jnp.arange(8 * slots)
            gates = jnp.where(hit, g.astype(BF16)[:, :, None], jnp.zeros((), BF16))
            z = dot(jnp.any(hit, axis=1).astype(BF16).T, x2).astype(BF16)
            z = lax.all_to_all(z.reshape(8, slots, depth), "ep", 0, 0).reshape(8 * slots, depth)
            u = (jax.nn.silu(dot(z, wg)) * dot(z, wu)).astype(BF16)
            out = dot(u, wd).astype(BF16).reshape(8, slots, depth)
            out = lax.all_to_all(out, "ep", 0, 0).reshape(8 * slots, depth)
            return dot(jnp.sum(gates, axis=1), out).astype(BF16)

        def pass_on():
            return pl.pallas_call(
                copy_kernel, out_shape=jax.ShapeDtypeStruct(y.shape, BF16), in_specs=[hbm], out_specs=hbm,
                scratch_shapes=[vmem(y.shape, BF16), dma((PIECES,)), dma((PIECES,))],
            )(y)

        y = lax.switch(over[0, 0], (pass_on, every_slot))
        return y.reshape(x.shape)

    tok = P("dp", "ep")
    return jax.shard_map(step, mesh=mesh, in_specs=(tok,) * 4 + (P("ep"),) * 3, out_specs=tok, check_vma=False)
```

```python
import functools

import jax
import jax.numpy as jnp
from jax import lax
from jax.experimental import pallas as pl
from jax.experimental.pallas import tpu as pltpu
from jax.sharding import PartitionSpec as P

MESH = pl.DeviceIdType.MESH
F32, BF16 = jnp.float32, jnp.bfloat16
PIECES = 4
COPIES = 2
ROWS = 176
NBUF = 4
DBUF = 2


def kernel(slots, groups, expert, slot, gate, x_hbm, wg, wu, wd, y_hbm, over,
           meta, mc, xv, xc, xf, mf, oc, oh, wt, counts, zz, stage, stagef, acc, hbuf, ro, rof,
           part, kbuf, dbuf,
           xsem, ksem, dsem, ysem, go,
           s_meta, s_x, s_own, s_rel, s_far, s_out, s_part,
           r_meta, r_x, r_z, r_zp, r_zn, r_rof, r_ro, r_part, s_count, r_count):
    S = slots
    T, D = xv.shape
    FF = hbuf.shape[1]
    KT, FT = kbuf.shape[1:]
    NT = dbuf.shape[2]
    C = D // PIECES
    HALF = 4 * S
    NF = FF // FT
    GU = 2 * NF * PIECES

    dp = lax.axis_index("dp")
    me = lax.axis_index("ep")
    z = lax.div(me, 2)
    k = lax.rem(me, 2)
    h = lax.div(me, 4)
    q = lax.rem(me, 4)
    side = lax.rem(z + h + 1, 2)
    mid = side == 0
    end = side == 1
    partner = 2 * z + 1 - k
    qp = partner - 4 * h
    other = 2 + 8 * h - 2 * z
    qo = other - 4 * h
    relay = 4 - 2 * h + k
    far_end = 6 - 6 * h + k
    base = h * HALF
    block = side * 2 + (1 - side) * (2 + k)

    def rows(i):
        return pl.ds(pl.multiple_of(i * S, 16), S)

    def cols(p):
        return pl.ds(pl.multiple_of(p * C, 128), C)

    def send(src, dst, ssem, rsem, dev):
        return pltpu.make_async_remote_copy(
            src_ref=src, dst_ref=dst, send_sem=ssem, recv_sem=rsem,
            device_id=(dp, dev), device_id_type=MESH)

    def recv(dst, rsem):
        pltpu.make_async_remote_copy(
            src_ref=dst, dst_ref=dst, send_sem=rsem, recv_sem=rsem,
            device_id=(dp, partner), device_id_type=MESH).wait_recv()

    def gu_copy(t, w, m):
        t = lax.rem(t, GU)
        r = pl.ds(pl.multiple_of(lax.div(t, 2 * NF) * KT, 128), KT)
        c = pl.ds(pl.multiple_of(lax.div(lax.rem(t, 2 * NF), 2) * FT, 128), FT)
        return w.at[r, c]

    def gu_start(t):
        s = lax.rem(t, NBUF)

        @pl.when(lax.rem(t, 2) == 0)
        def _():
            pltpu.make_async_copy(gu_copy(t, wg, 0), kbuf.at[s], ksem.at[s]).start()

        @pl.when(lax.rem(t, 2) == 1)
        def _():
            pltpu.make_async_copy(gu_copy(t, wu, 1), kbuf.at[s], ksem.at[s]).start()

    def gu_wait(t):
        s = lax.rem(t, NBUF)
        pltpu.make_async_copy(gu_copy(t, wg, 0), kbuf.at[s], ksem.at[s]).wait()
        return s

    def dn_copy(t):
        s = lax.rem(t, DBUF)
        tile = pl.ds(pl.multiple_of(lax.rem(t, PIECES) * NT, 128), NT)
        return pltpu.make_async_copy(wd.at[:, tile], dbuf.at[s], dsem.at[s])

    xload = [pltpu.make_async_copy(x_hbm.at[:, cols(p)], xv.at[:, cols(p)], xsem.at[p])
             for p in range(PIECES)]
    for c in xload:
        c.start()
    for t in range(NBUF):
        gu_start(jnp.int32(t))
    for t in range(DBUF):
        dn_copy(jnp.int32(t)).start()

    barrier = pltpu.get_barrier_semaphore()

    def greet(d):
        pl.semaphore_signal(barrier, inc=1, device_id=d, device_id_type=MESH)

    peers = [(dp, d) for d in (partner, other, other + 1, relay)]
    peers += [(lax.rem(dp + d, groups), me) for d in range(1, groups)]
    for d in peers:
        greet(d)
    pl.when(mid)(lambda: greet((dp, far_end)))

    def onehot(m, first):
        idx = m[...].astype(jnp.int32) - first
        r = lax.broadcasted_iota(jnp.int32, (HALF, T), 0)
        hit = (r == idx[0:1, :]) | (r == idx[1:2, :])
        return jnp.where(hit, 1.0, 0.0).astype(BF16)

    def by_token(m):
        return jnp.transpose(jnp.concatenate([m[...], jnp.zeros((120, T), F32)], axis=0))

    def weights_of(mt, first):
        idx = mt.astype(jnp.int32) - first
        r = lax.broadcasted_iota(jnp.int32, (T, HALF), 1)
        w = jnp.where(r == idx[:, 0:1], mt[:, 2:3], 0.0)
        w = jnp.where(r == idx[:, 1:2], mt[:, 3:4], w)
        return w.astype(BF16)

    def dot(a, b):
        return jnp.dot(a, b, preferred_element_type=F32)

    meta[...] = jnp.zeros_like(meta)
    meta[0:2, :] = jnp.where(slot[...] < S, expert[...] * S + slot[...], -100000).astype(F32)
    meta[2:4, :] = gate[...]
    oh[0] = onehot(meta, base)

    far = expert[...] - 4 * (1 - h)
    there = (far >= 0) & (far < 4) & (slot[...] < S)
    mc[...] = jnp.zeros_like(mc)
    mc[0:2, :] = jnp.where(there, far, -4).astype(F32)
    mc[2:4, :] = jnp.where(there, slot[...], 0).astype(F32)
    mc[4:6, :] = gate[...]
    cross = jnp.max(jnp.where(there, 1.0, 0.0), axis=0, keepdims=True)
    before = lax.broadcasted_iota(jnp.int32, (T, T), 0) < lax.broadcasted_iota(jnp.int32, (T, T), 1)
    rank = dot(jnp.broadcast_to(cross, (8, T)).astype(BF16), jnp.where(before, 1.0, 0.0).astype(BF16))[0:1, :]
    rank = jnp.where(cross > 0, rank, -1.0)
    meta[4:5, :] = rank
    oc[...] = jnp.where(lax.broadcasted_iota(jnp.int32, (T, T), 0) == rank.astype(jnp.int32), 1.0, 0.0).astype(BF16)
    m = lax.dot_general(mc[...].astype(BF16), oc[...], (((1,), (1,)), ((), ())), preferred_element_type=F32)
    mc[0:2, :] = m[0:2, :] * S + m[2:4, :]
    mc[2:4, :] = m[4:6, :]
    counts[0] = jnp.broadcast_to(jnp.sum(cross, axis=1, keepdims=True), counts.shape[1:])
    pl.semaphore_wait(barrier, len(peers) + 1 - side)

    send_meta = send(mc, mf.at[side], s_meta, r_meta.at[side], relay)

    def send_x(p):
        return send(xc.at[:, cols(p)], xf.at[side, :, cols(p)], s_x.at[p], r_x.at[side, p], relay)

    def own_copy(p):
        return send(stage.at[rows(qp), cols(p)], zz.at[1, rows(block), cols(p)], s_own.at[0, p], r_zp.at[p], partner)

    def near_copy(j, p):
        f = (1 - side) * lax.rem(k + j, 2)
        r = (1 - side) * 3 + side * (2 + k)
        return send(stage.at[rows(qo + j), cols(p)], zz.at[f, rows(r), cols(p)], s_own.at[1 + j, p],
                    r_zn.at[k, p], other + j)

    send_meta.start()
    def pack_x(p):
        xc[:, cols(p)] = dot(oc[0:ROWS, :], xv[:, cols(p)]).astype(BF16)

    for p in range(PIECES):
        xload[p].wait()

        @pl.when(mid)
        def _(p=p):
            pack_x(p)
            send_x(p).start()

    for p in range(PIECES):
        stage[:, cols(p)] = dot(oh[0], xv[:, cols(p)]).astype(BF16)
        if p < 1:
            pl.when(mid)(near_copy(k, p).start)
        own_copy(p).start()

        @pl.when(end)
        def _(p=p):
            for j in range(2):
                near_copy(j, p).start()

        zz[1 - side, rows(block), cols(p)] = stage[rows(q), cols(p)]

    @pl.when(end)
    def _():
        for p in range(PIECES):
            pack_x(p)

    def count_copy(src, dst, i, dev):
        return pltpu.make_async_remote_copy(
            src_ref=counts.at[src], dst_ref=counts.at[dst], send_sem=s_count.at[i], recv_sem=r_count.at[dst],
            device_id=dev, device_id_type=MESH)

    count_half = [count_copy(0, 1, 1, (dp, partner)), count_copy(0, 2 + k, 2, (dp, other)),
                  count_copy(0, 2 + k, 3, (dp, other + 1))]
    count_over = [count_copy(4, 5, 4, (dp, relay)), count_copy(4, 5, 5, (dp, far_end))]
    count_dp = [count_copy(6, 6 + d, 5 + d, (lax.rem(dp + d, groups), me)) for d in range(1, groups)]
    for c in count_half:
        c.start()

    def largest(i, slots):
        top = counts[i]
        for d in slots:
            recv(counts.at[d], r_count.at[d])
            top = jnp.maximum(top, counts[d])
        return top

    def count_far():
        counts[4] = largest(0, (1, 2, 3))

        @pl.when(mid)
        def _():
            for c in count_over:
                c.start()

    def count_group():
        counts[6] = largest(4, (5,))
        for c in count_dp:
            c.start()

    def count_all():
        top = largest(6, range(7, 6 + groups))
        over[0, 0] = (jnp.max(top) > ROWS).astype(jnp.int32)

    def relay_copies(f, p):
        return [send(stagef.at[f, rows(qd), cols(p)], zz.at[f, rows(k), cols(p)], s_rel.at[f, j, p],
                     r_z.at[f, k, p], dev)
                for j, (qd, dev) in enumerate(((qp, partner), (qo, other), (qo + 1, other + 1)))]

    def relay_head(f):
        recv(mf.at[f], r_meta.at[f])
        oh[1 + f] = onehot(mf.at[f], 0)

    def relay_piece(f, p):
        recv(xf.at[f, :, cols(p)], r_x.at[f, p])
        stagef[f, :, cols(p)] = dot(oh[1 + f, :, 0:ROWS], xf[f, :, cols(p)]).astype(BF16)
        for c in relay_copies(f, p):
            c.start()
        zz[f, rows(k), cols(p)] = stagef[f, rows(q), cols(p)]

    def await_z(f, p):
        recv(zz.at[f, rows(1 - k), cols(p)], r_z.at[f, 1 - k, p])

        @pl.when(end)
        def _():
            recv(zz.at[f, rows(k), cols(p)], r_z.at[f, k, p])

        @pl.when(mid & (f == 0))
        def _():
            for j in range(2):
                recv(zz.at[f, rows(2 + j), cols(p)], r_zn.at[j, p])

        @pl.when(mid & (f == 1))
        def _():
            recv(zz.at[f, rows(3 - k), cols(p)], r_zp.at[p])

        @pl.when(end & (f == 1))
        def _():
            recv(zz.at[f, rows(2), cols(p)], r_zp.at[p])

        @pl.when(end)
        def _():
            recv(zz.at[f, rows(3), cols(p)], r_zn.at[lax.rem(k + f, 2), p])

    def ft(c):
        return pl.ds(pl.multiple_of(c * FT, 128), FT)

    def gu_next(t):
        @pl.when(t + NBUF < 2 * GU)
        def _():
            gu_start(t + NBUF)

    def gu_piece(f, p):
        t0 = f * GU + p * 2 * NF
        zp = zz.at[f, :, cols(p)]

        @pl.loop(0, NF)
        def _(i):
            c = ft(i)
            t = t0 + 2 * i
            sg, su = gu_wait(t), gu_wait(t + 1)
            g = dot(zp[...], kbuf[sg])
            if p == 0:
                acc[0, :, c] = g
                acc[1, :, c] = dot(zp[...], kbuf[su])
            elif p < PIECES - 1:
                acc[0, :, c] += g
                acc[1, :, c] += dot(zp[...], kbuf[su])
            else:
                g = acc[0, :, c] + g
                acc[0, :, c] = g * jax.nn.sigmoid(g)
                hbuf[:, c] = (acc[0, :, c] * (acc[1, :, c] + dot(zp[...], kbuf[su]))).astype(BF16)
            gu_next(t)
            gu_next(t + 1)

    def dn_piece(f, p):
        t = f * PIECES + p
        dn_copy(t).wait()
        zz[f, :, cols(p)] = dot(hbuf[...], dbuf[lax.rem(t, DBUF)]).astype(BF16)

        @pl.when(t + DBUF < 2 * PIECES)
        def _():
            dn_copy(t + DBUF).start()

    def out_far(f, p, start):
        def to(kk, dev):
            return send(zz.at[f, rows(kk), cols(p)], rof.at[f, rows(q), cols(p)], s_far.at[f, kk, p],
                        r_rof.at[f, q, p], dev)

        @pl.when(mid)
        def _():
            c = to(1 - k, partner)
            if start:
                c.start()
                rof[f, rows(q), cols(p)] = zz[f, rows(k), cols(p)]
            else:
                c.wait_send()

        @pl.when(end)
        def _():
            for kk in range(2):
                c = to(kk, other + kk)
                c.start() if start else c.wait_send()

    def out_chip(p):
        r = side * 2 + (1 - side) * (3 - k)
        return send(zz.at[1, rows(r), cols(p)], ro.at[rows(q), cols(p)], s_out.at[0, p], r_ro.at[q, p], partner)

    def out_other(j, p):
        f = side * lax.rem(k + j, 2)
        r = side * 3 + (1 - side) * (2 + j)
        return send(zz.at[f, rows(r), cols(p)], ro.at[rows(q), cols(p)], s_out.at[1 + j, p],
                    r_ro.at[q, p], other + j)

    def send_part(f, p):
        dev = relay if f == 0 else far_end
        return send(xf.at[f, :, cols(p)], part.at[:, cols(p)], s_part.at[f, p], r_part.at[p], dev)

    def combine_piece(f, p):
        for qq in (qp, qo, qo + 1):
            recv(rof.at[f, rows(qq), cols(p)], r_rof.at[f, qq, p])
        xf[f, :, cols(p)] = dot(wt[1 + f, 0:ROWS, :], rof[f, :, cols(p)]).astype(BF16)
        send_part(f, p).start()

    pl.when(mid)(lambda: relay_head(0))

    @pl.loop(0, 2)
    def _(f):
        for p in range(PIECES):
            if p < 3:
                @pl.when(mid & ((f == 0) | (p < 2)))
                def _(p=p):
                    early = min(p, 1)
                    relay_piece(f, (p + early) * (1 - f) + (p + 2) * f)
                    if p != 2:
                        pl.when(f == 0)(near_copy(k, 2 * p + 1).start)

            if p < 2:
                pl.when(mid & (f == 1))(near_copy(1 - k, p + 2).start)

            if p == 1:
                @pl.when(end & (f == 0))
                def _():
                    pl.semaphore_wait(go, 1)
                    for pp in range(PIECES):
                        send_x(pp).start()

                @pl.when(mid & (f == 1))
                def _():
                    wt[1] = weights_of(by_token(mf.at[0]), 0)

            if p == 2:
                @pl.when(mid & (f == 1))
                def _():
                    for pp in range(PIECES):
                        for j in range(2):
                            out_other(j, pp).start()

            if p == 3:
                @pl.when(mid & (f == 0))
                def _():
                    for pp in range(2):
                        near_copy(1 - k, pp).start()

                @pl.when(mid & (f == 1))
                def _():
                    wt[2] = weights_of(by_token(mf.at[1]), 0)

            if p > 0:
                @pl.when(mid & (f == 1))
                def _(p=p):
                    combine_piece(0, p - 1)

            await_z(f, p)
            if p == 0:
                @pl.when(mid & (f == 0))
                def _():
                    relay_piece(0, 1)
                    pl.semaphore_signal(go, inc=1, device_id=(dp, far_end), device_id_type=MESH)
                    near_copy(k, 2).start()

            gu_piece(f, p)

        @pl.when(mid & (f == 1))
        def _():
            combine_piece(0, 3)

        pl.when(f == 0)(count_far)
        pl.when(f == 1)(count_group)

        @pl.loop(0, PIECES)
        def _(p):
            @pl.when(mid & (f == 0) & (p == 1))
            def _():
                relay_head(1)
                relay_piece(1, 0)

            @pl.when(mid & (f == 0) & (p == 3))
            def _():
                relay_piece(1, 1)

            @pl.when(mid & (f == 1) & (p == 3))
            def _():
                combine_piece(1, 0)

            dn_piece(f, p)
            out_far(f, p, True)

            @pl.when(f == 1)
            def _():
                out_chip(p).start()

            @pl.when(f == 1 - side)
            def _():
                ro[rows(q), cols(p)] = zz[f, rows(block), cols(p)]

        @pl.when(end)
        def _():
            for p in range(PIECES):
                out_other(lax.rem(k + f, 2), p).start()

    @pl.when(mid)
    def _():
        for p in range(1, PIECES):
            combine_piece(1, p)

    count_all()
    mt = by_token(meta)
    wt[0] = weights_of(mt, base)
    oc[...] = jnp.where(lax.broadcasted_iota(jnp.int32, (T, T), 1) == mt[:, 4:5].astype(jnp.int32), 1.0, 0.0).astype(BF16)
    send_meta.wait_send()
    for p in range(PIECES):
        send_x(p).wait_send()
    ycopy = [pltpu.make_async_copy(xv.at[:, cols(p)], y_hbm.at[:, cols(p)], ysem.at[p]) for p in range(PIECES)]
    for p in range(PIECES):
        recv(ro.at[rows(qp), cols(p)], r_ro.at[qp, p])
        for j in range(2):
            recv(ro.at[rows(qo + j), cols(p)], r_ro.at[qo + j, p])
        acc[0, 0:T, cols(p)] = dot(wt[0], ro[:, cols(p)])

    for p in range(PIECES):
        recv(part.at[:, cols(p)], r_part.at[p])
        xv[:, cols(p)] = (acc[0, 0:T, cols(p)] + dot(oc[:, 0:ROWS], part[:, cols(p)])).astype(BF16)
        ycopy[p].start()

    for p in range(PIECES):
        for c in (own_copy(p), near_copy(0, p), near_copy(1, p), out_chip(p), out_other(0, p), out_other(1, p)):
            c.wait_send()
        for f in range(2):
            out_far(f, p, False)

    @pl.when(mid)
    def _():
        for p in range(PIECES):
            for f in range(2):
                for c in relay_copies(f, p):
                    c.wait_send()
                send_part(f, p).wait_send()

    for c in (*count_half, *count_dp):
        c.wait_send()

    @pl.when(mid)
    def _():
        for c in count_over:
            c.wait_send()

    for c in ycopy:
        c.wait()


def copy_kernel(src, dst, buf, isem, osem):
    n = buf.shape[0] // COPIES
    parts = [pl.ds(i * n, n) for i in range(COPIES)]
    load = [pltpu.make_async_copy(src.at[r], buf.at[r], isem.at[i]) for i, r in enumerate(parts)]
    save = [pltpu.make_async_copy(buf.at[r], dst.at[r], osem.at[i]) for i, r in enumerate(parts)]
    for c in load:
        c.start()
    for a, b in zip(load, save):
        a.wait()
        b.start()
    for c in save:
        c.wait()


def solution(mesh):
    def step(x, expert, slot, gate, w_gate, w_up, w_down):
        tokens, depth = x.shape[2:]
        ff = w_gate.shape[2]
        top = expert.shape[3]
        slots = 5 * tokens * top // (4 * 8)
        half = 4 * slots
        dma = pltpu.SemaphoreType.DMA
        vmem = pltpu.VMEM
        hbm = pl.BlockSpec(memory_space=pl.ANY)
        routing = [v.reshape(tokens, top) for v in (expert, slot, gate)]
        x2, wg, wu, wd = x.reshape(tokens, depth), w_gate[0], w_up[0], w_down[0]
        groups = mesh.shape["dp"]
        y, over = pl.pallas_call(
            functools.partial(kernel, slots, groups),
            out_shape=(jax.ShapeDtypeStruct((tokens, depth), BF16), jax.ShapeDtypeStruct((1, 1), jnp.int32)),
            in_specs=[pl.BlockSpec(memory_space=pltpu.VMEM)] * 3 + [hbm] * 4,
            out_specs=(hbm, pl.BlockSpec(memory_space=pltpu.SMEM)),
            scratch_shapes=[
                vmem((8, tokens), F32),
                vmem((8, tokens), F32),
                vmem((tokens, depth), BF16),
                vmem((ROWS, depth), BF16),
                vmem((2, ROWS, depth), BF16),
                vmem((2, 8, tokens), F32),
                vmem((tokens, tokens), BF16),
                vmem((3, half, tokens), BF16),
                vmem((3, tokens, half), BF16),
                vmem((12, 8, 128), F32),
                vmem((2, half, depth), BF16),
                vmem((half, depth), BF16),
                vmem((2, half, depth), BF16),
                vmem((2, half, ff), F32),
                vmem((half, ff), BF16),
                vmem((half, depth), BF16),
                vmem((2, half, depth), BF16),
                vmem((ROWS, depth), BF16),
                vmem((NBUF, depth // PIECES, ff // 2), BF16),
                vmem((DBUF, ff, depth // PIECES), BF16),
                dma((PIECES,)), dma((NBUF,)), dma((DBUF,)), dma((PIECES,)),
                pltpu.SemaphoreType.REGULAR,
                dma, dma((PIECES,)), dma((3, PIECES)), dma((2, 3, PIECES)),
                dma((2, 2, PIECES)), dma((3, PIECES)), dma((2, PIECES)),
                dma((2,)), dma((2, PIECES)), dma((2, 2, PIECES)), dma((PIECES,)), dma((2, PIECES)),
                dma((2, 4, PIECES)), dma((4, PIECES)), dma((PIECES,)), dma((11,)), dma((11,)),
            ],
            compiler_params=pltpu.CompilerParams(
                collective_id=0, has_side_effects=True, vmem_limit_bytes=67043328),
        )(*(v.T for v in routing), x2, wg, wu, wd)

        def dot(a, b):
            return jnp.dot(a, b, preferred_element_type=F32)

        def every_slot():
            e, c, g = routing
            place = jnp.where(c < slots, e * slots + c, -1)
            hit = place[:, :, None] == jnp.arange(8 * slots)
            gates = jnp.where(hit, g.astype(BF16)[:, :, None], jnp.zeros((), BF16))
            z = dot(jnp.any(hit, axis=1).astype(BF16).T, x2).astype(BF16)
            z = lax.all_to_all(z.reshape(8, slots, depth), "ep", 0, 0).reshape(8 * slots, depth)
            u = (jax.nn.silu(dot(z, wg)) * dot(z, wu)).astype(BF16)
            out = dot(u, wd).astype(BF16).reshape(8, slots, depth)
            out = lax.all_to_all(out, "ep", 0, 0).reshape(8 * slots, depth)
            return dot(jnp.sum(gates, axis=1), out).astype(BF16)

        def pass_on():
            return pl.pallas_call(
                copy_kernel, out_shape=jax.ShapeDtypeStruct(y.shape, BF16), in_specs=[hbm], out_specs=hbm,
                scratch_shapes=[vmem(y.shape, BF16), dma((COPIES,)), dma((COPIES,))],
            )(y)

        y = lax.switch(over[0, 0], (pass_on, every_slot))
        return y.reshape(x.shape)

    tok = P("dp", "ep")
    return jax.shard_map(step, mesh=mesh, in_specs=(tok,) * 4 + (P("ep"),) * 3, out_specs=tok, check_vma=False)
```
